32 devices in a mesh: dp: 8 (over z, core), fsdp: 4 (over y, x).
Axes of the slice: x: 2, y: 2, z: 4, core: 2. Of those that a mesh axis runs over, the one named last changes fastest.
Arguments:
- features: bfloat16 [4, 8, 32, 32, 512], P('fsdp', None, 'dp'), may hold values from -6 to 6
- conv_weight: bfloat16 [3, 3, 512, 8], replicated, may hold values from -0.046875 to 0.046875
- vae_noise: float32 [8, 4, 4096], P('dp', 'fsdp'), may hold values from -6 to 6
- flips: int32 [8, 4, 4], P('dp', 'fsdp'), may hold values from 0 to 1
- crops: int32 [8, 4, 4, 2], P('dp', 'fsdp'), may hold values from 0 to 4
- tsteps: int32 [8, 4, 4], P('dp', 'fsdp'), may hold values from 0 to 999
- diffusion_noise: float32 [8, 4, 4, 4096], P('dp', 'fsdp'), may hold values from -6 to 6
- selected: int32 [8, 4], P('dp', 'fsdp'), may hold values from 0 to 1, as said below
- w_patch: bfloat16 [16, 384], replicated, may hold values from -1.5 to 1.5
- w_time: bfloat16 [256, 384], replicated, may hold values from -0.375 to 0.375
- w_ada: bfloat16 [384, 1152], replicated, may hold values from -0.3125 to 0.3125
- w_fc1: bfloat16 [384, 1536], P(None, 'fsdp'), may hold values from -1 to 1
- w_fc2: bfloat16 [384, 1536], P(None, 'fsdp'), may hold values from -1 to 1
- w_final: bfloat16 [384, 16], replicated, may hold values from -0.3125 to 0.3125
- noise_fc1: float32 [384, 1536], P(None, 'fsdp'), may hold values from -6 to 6
- noise_fc2: float32 [384, 1536], P(None, 'fsdp'), may hold values from -6 to 6
Outputs:
- update_fc1: float32 [384, 1536], P(None, 'fsdp')
- update_fc2: float32 [384, 1536], P(None, 'fsdp')
- mean_loss: float32 [], replicated
- latent_moments: float32 [8, 4, 8192], P('dp', 'fsdp')
The draws below stay inside these ranges and needn't reach their ends.
Inputs may be any that keep to these rules, and one draw needn't show every extreme that they name: `selected`: exactly 16 slots are 1.
All inputs are finite; a program needn't handle non-finite values.
Results may differ from the reference program's by a relative error of at most 0.00091.
Values may be sent and summed in bfloat16 or wider, within the bound.
No kernel may reach another device: no remote copies, remote signals or barrier semaphores. Data moves between devices by JAX's collectives and lax.ppermute only.
A program may use at most 64 MiB of HBM per device.

```python
import math
from functools import partial
import jax
import jax.numpy as jnp
from jax import lax

D = 384
FF = 1536
FCH = 512
FREQ = 256
LAT = 32
LC = 4
AUG = 4
TSTEPS = 1000
SLOTS = 8
SELECTED = 16
N_FSDP = 4


def scaled_columns(key, row_count, col_count, fan_in):
    base_values = jnp.clip(jax.random.normal(key, (row_count, col_count), jnp.float32), -6.0, 6.0)
    spread = jnp.exp(jax.random.uniform(jax.random.fold_in(key, 7), (col_count,), jnp.float32, -1.15, 1.15))
    return jnp.clip(base_values * spread[None, :] / math.sqrt(fan_in), -1.0, 1.0)


def draw_w_fc1(key, part):
    return scaled_columns(key, D, FF, D).astype(jnp.bfloat16)


def draw_w_fc2(key, part):
    return scaled_columns(key, D, FF, FF).astype(jnp.bfloat16)


def draw_diffusion_noise(key, part):
    full_shape = (SLOTS, N_FSDP, AUG, LAT * LAT * LC)
    return jnp.clip(jax.random.normal(key, full_shape, jnp.float32), -6.0, 6.0)


def draw_selected(key, part):
    shuffled = jax.random.permutation(key, SLOTS * N_FSDP)
    return (shuffled < SELECTED).astype(jnp.int32).reshape(SLOTS, N_FSDP)


def set_ends(drawn, stream_key, low, top_value):
    longest = drawn.shape.index(max(drawn.shape))
    spots = []
    for shift in (0, 1):
        where = [jax.random.randint(jax.random.fold_in(stream_key, axis), (), 0, length) for axis, length in enumerate(drawn.shape)]
        where[longest] = (where[longest] + shift) % drawn.shape[longest]
        spots.append(tuple(where))
    return drawn.at[spots[0]].set(low).at[spots[1]].set(top_value)


def steps_of(own_key, shape, cuts, least, largest):
    def one(position, blocks):
        draws = jax.random.uniform(jax.random.fold_in(jax.random.fold_in(own_key, 6), position), (blocks,), jnp.float32, least / len(cuts), largest / len(cuts))
        return jnp.repeat(jnp.exp(draws), shape[position] // blocks).reshape((-1,) + (1,) * (len(shape) - position - 1))

    loudness = one(*cuts[0])
    for cut in cuts[1:]:
        loudness = loudness * one(*cut)
    return loudness


def scatter_about(key, dims, deviation, reach, cuts=(), kind=jnp.bfloat16):
    array = jax.random.normal(key, dims, jnp.float32) * deviation
    if len(cuts) > 0:
        array = steps_of(key, dims, cuts, -0.22, 0.18) * array
    return jnp.clip(array, min=-reach, max=reach).astype(kind)


def setup_inputs(seed: int = 0) -> dict:
    keys = jax.random.split(jax.random.key(seed), 17)
    features = scatter_about(keys[0], (N_FSDP, SLOTS, LAT, LAT, FCH), 1.0, 6.0, ((0, 4), (2, 8)))
    conv_weight = scatter_about(keys[1], (3, 3, FCH, 2 * LC), (36 * FCH) ** -0.5, 0.046875)
    vae_noise = scatter_about(keys[2], (SLOTS, N_FSDP, LAT * LAT * LC), 1.0, 6.0, ((0, 8), (1, 4)), jnp.float32)
    flips = set_ends(jax.random.randint(keys[3], (SLOTS, N_FSDP, AUG), 0, 2), jax.random.fold_in(keys[3], 1), 0, 1).astype(jnp.int32)
    crops = set_ends(jax.random.randint(keys[4], (SLOTS, N_FSDP, AUG, 2), 0, 5), jax.random.fold_in(keys[4], 1), 0, 4).astype(jnp.int32)
    tsteps = set_ends(jax.random.randint(keys[5], (SLOTS, N_FSDP, AUG), 0, TSTEPS), jax.random.fold_in(keys[5], 1), 0, TSTEPS - 1).astype(jnp.int32)
    diffusion_noise = draw_diffusion_noise(jax.random.fold_in(keys[16], 71), 0)
    selected = draw_selected(jax.random.fold_in(keys[16], 71), 0)
    w_patch = scatter_about(keys[8], (4 * LC, D), (4 * LC) ** -0.5, 1.5)
    w_time = scatter_about(keys[9], (FREQ, D), FREQ ** -0.5, 0.375)
    w_ada = scatter_about(keys[10], (D, 3 * D), D ** -0.5, 0.3125)
    w_fc1 = draw_w_fc1(jax.random.fold_in(keys[16], 71), 0)
    w_fc2 = draw_w_fc2(jax.random.fold_in(keys[16], 71), 0)
    w_final = scatter_about(keys[13], (D, 4 * LC), D ** -0.5, 0.3125)
    noise_fc1 = scatter_about(keys[14], (D, FF), 1.0, 6.0, ((1, 4),), jnp.float32)
    noise_fc2 = scatter_about(keys[15], (D, FF), 1.0, 6.0, ((1, 4),), jnp.float32)
    return dict(features=features, conv_weight=conv_weight, vae_noise=vae_noise, flips=flips, crops=crops, tsteps=tsteps, diffusion_noise=diffusion_noise, selected=selected, w_patch=w_patch, w_time=w_time, w_ada=w_ada, w_fc1=w_fc1, w_fc2=w_fc2, w_final=w_final, noise_fc1=noise_fc1, noise_fc2=noise_fc2)


clip_offset = 1e-05
noise_weight = 16.0
norm_epsilon = 1e-06

def layer_norm(values):
    center = values - lax.optimization_barrier(jnp.mean(values, axis=-1, keepdims=True))
    variance = lax.optimization_barrier(jnp.mean(center * center, axis=-1, keepdims=True))
    return center * lax.rsqrt(variance + norm_epsilon)

def position_table(side_cells, width):
    quarter = width // 4
    frequency = 1.0 / 10000.0 ** (jnp.arange(quarter, dtype=jnp.float32) / quarter)
    positions = jnp.arange(side_cells, dtype=jnp.float32)
    angles = positions[:, None] * frequency[None, :]
    line_table = jnp.concatenate([jnp.sin(angles), jnp.cos(angles)], axis=1)
    row_part = jnp.repeat(line_table, side_cells, axis=0)
    col_part = jnp.tile(line_table, (side_cells, 1))
    return jnp.concatenate([row_part, col_part], axis=1)

def time_features(steps_in, width):
    half_width = width // 2
    rates = jnp.exp(-math.log(10000.0) * jnp.arange(half_width, dtype=jnp.float32) / half_width)
    phases = steps_in.astype(jnp.float32)[:, None] * rates[None, :]
    return jnp.concatenate([jnp.cos(phases), jnp.sin(phases)], axis=1)

def alpha_bars(steps_in, horizon):
    beta_table = jnp.linspace(0.0001, 0.02, horizon, dtype=jnp.float32)
    alpha_bar = jnp.cumprod(1.0 - beta_table)
    matches = jnp.arange(horizon, dtype=jnp.int32)[None, :] == steps_in.astype(jnp.int32)[:, None]
    return lax.optimization_barrier(jnp.sum(jnp.where(matches, alpha_bar[None, :], 0.0), axis=1))

def augment(latent, mirror, crop_at):
    side_cells = latent.shape[0]
    mirrored = jnp.where(mirror == 1, latent[:, ::-1, :], latent)
    padded = jnp.pad(mirrored, ((2, 2), (2, 2), (0, 0)))
    starts = (crop_at[0].astype(jnp.int32), crop_at[1].astype(jnp.int32), jnp.int32(0))
    return lax.dynamic_slice(padded, starts, (side_cells, side_cells, latent.shape[2]))

def patchify(grid):
    views_count = grid.shape[0]
    half_side = grid.shape[1] // 2
    channels = grid.shape[3]
    blocks = grid.reshape(views_count, half_side, 2, half_side, 2, channels)
    blocks = blocks.transpose(0, 1, 3, 2, 4, 5)
    return blocks.reshape(views_count * half_side * half_side, 4 * channels)

def conv_moments(padded, kernel):
    image_count, padded_rows, side_cells, channels = padded.shape
    out_width = kernel.shape[3]
    tap_matrix = kernel.transpose(2, 0, 1, 3).reshape(channels, 9 * out_width)
    tap_values = jnp.dot(padded.reshape(-1, channels), tap_matrix, preferred_element_type=jnp.float32)
    tap_values = tap_values.reshape(image_count, padded_rows, side_cells, 3, 3, out_width)
    tap_values = jnp.pad(tap_values, ((0, 0), (0, 0), (1, 1), (0, 0), (0, 0), (0, 0)))
    out_rows = padded_rows - 2
    summed = jnp.zeros((image_count, out_rows, side_cells, out_width), jnp.float32)
    for row_tap in range(3):
        for col_tap in range(3):
            summed = summed + tap_values[:, row_tap:row_tap + out_rows, col_tap:col_tap + side_cells, row_tap, col_tap, :]
    return summed

def example_terms(mean_part, logvar, vae_eps, mirror, crop_at, steps_in, noise, weights):
    w_patch, w_time, w_ada, w_fc1, w_fc2, w_final = weights
    side_cells = mean_part.shape[0]
    channels = mean_part.shape[2]
    views_count = mirror.shape[0]
    width = w_fc1.shape[0]
    latent = mean_part + jnp.exp(0.5 * logvar) * vae_eps.reshape(mean_part.shape)
    augmented = jax.vmap(augment, in_axes=(None, 0, 0))(latent, mirror, crop_at)
    alpha_bar = alpha_bars(steps_in, TSTEPS)
    noise_grid = noise.reshape(views_count, side_cells, side_cells, channels)
    keep_part = jnp.sqrt(alpha_bar)[:, None, None, None]
    blend_part = jnp.sqrt(1.0 - alpha_bar)[:, None, None, None]
    noised = keep_part * augmented + blend_part * noise_grid
    patches = patchify(noised).astype(jnp.bfloat16)
    target = patchify(noise_grid)
    half_side = side_cells // 2
    per_view = half_side * half_side
    tokens = jnp.dot(patches, w_patch, preferred_element_type=jnp.float32)
    tokens = tokens + jnp.tile(position_table(half_side, width), (views_count, 1))
    stamp = time_features(steps_in, w_time.shape[0]).astype(jnp.bfloat16)
    conditioning = jax.nn.silu(jnp.dot(stamp, w_time, preferred_element_type=jnp.float32))
    modulation = jnp.dot(conditioning.astype(jnp.bfloat16), w_ada, preferred_element_type=jnp.float32)
    offset_rows = jnp.repeat(modulation[:, :width], per_view, axis=0)
    scale_rows = jnp.repeat(modulation[:, width:2 * width], per_view, axis=0)
    gate_rows = jnp.repeat(modulation[:, 2 * width:], per_view, axis=0)
    modulated = (layer_norm(tokens) * (1.0 + scale_rows) + offset_rows).astype(jnp.bfloat16)
    preact = jnp.dot(modulated, w_fc1, preferred_element_type=jnp.float32)
    hidden, gelu_back = jax.vjp(partial(jax.nn.gelu, approximate=True), preact)
    hidden_low = hidden.astype(jnp.bfloat16)
    branch = lax.dot_general(hidden_low, w_fc2, (((1,), (1,)), ((), ())), preferred_element_type=jnp.float32)
    mixed_rows = tokens + gate_rows * branch
    final_norm, norm_back = jax.vjp(layer_norm, mixed_rows)
    final_low = final_norm.astype(jnp.bfloat16)
    predicted = jnp.dot(final_low, w_final, preferred_element_type=jnp.float32)
    residue = predicted - target
    entries = residue.shape[0] * residue.shape[1]
    loss_value = jnp.sum(residue * residue) / entries
    grad_pred = (residue * (2.0 / entries)).astype(jnp.bfloat16)
    grad_final = lax.dot_general(grad_pred, w_final, (((1,), (1,)), ((), ())), preferred_element_type=jnp.float32)
    grad_mixed = norm_back(grad_final)[0]
    grad_branch = (gate_rows * grad_mixed).astype(jnp.bfloat16)
    grad_fc2 = lax.dot_general(grad_branch, hidden_low, (((0,), (0,)), ((), ())), preferred_element_type=jnp.float32)
    grad_hidden = jnp.dot(grad_branch, w_fc2, preferred_element_type=jnp.float32)
    grad_pre = gelu_back(grad_hidden)[0].astype(jnp.bfloat16)
    grad_fc1 = lax.dot_general(modulated, grad_pre, (((0,), (0,)), ((), ())), preferred_element_type=jnp.float32)
    return (loss_value, grad_fc1, grad_fc2)

def clip_pair(grad_fc1, grad_fc2):
    squares = jnp.sum(grad_fc1 * grad_fc1) + jnp.sum(grad_fc2 * grad_fc2)
    root_mean = jnp.sqrt(squares / (grad_fc1.size + grad_fc2.size))
    factor = 1.0 / (root_mean + clip_offset)
    return (grad_fc1 * factor, grad_fc2 * factor)

def selected_terms(chosen, mean_part, logvar, vae_eps, mirror, crop_at, steps_in, noise, weights):

    def compute():
        loss_value, grad_fc1, grad_fc2 = example_terms(mean_part, logvar, vae_eps, mirror, crop_at, steps_in, noise, weights)
        clipped_fc1, clipped_fc2 = clip_pair(grad_fc1, grad_fc2)
        return (loss_value, clipped_fc1, clipped_fc2)

    def skipped():
        zeros = jnp.zeros((weights[3].shape[0], weights[3].shape[1]), jnp.float32)
        return (jnp.zeros((), jnp.float32), zeros, zeros)
    return lax.cond(chosen == 1, compute, skipped)

def reference(features, conv_weight, vae_noise, flips, crops, tsteps, diffusion_noise, selected, w_patch, w_time, w_ada, w_fc1, w_fc2, w_final, noise_fc1, noise_fc2):
    group_count = features.shape[0]
    slot_count = features.shape[1]
    side_cells = features.shape[2]
    images = features.reshape(group_count * slot_count, side_cells, side_cells, features.shape[4])

    def one_image(image):
        padded = jnp.pad(image, ((1, 1), (0, 0), (0, 0)))[None]
        return conv_moments(padded, conv_weight)[0]
    moments = lax.map(one_image, images)
    latent_moments = jnp.swapaxes(moments.reshape(group_count, slot_count, -1), 0, 1)

    def reorder(values):
        return jnp.swapaxes(values, 0, 1).reshape((group_count * slot_count,) + values.shape[2:])
    inputs = (moments, reorder(vae_noise), reorder(flips), reorder(crops), reorder(tsteps), reorder(diffusion_noise), reorder(selected))
    weights = (w_patch, w_time, w_ada, w_fc1, w_fc2, w_final)
    channels = conv_weight.shape[3] // 2

    def accumulate(running, item):
        moment, vae_eps, mirror, crop_at, steps_in, noise, chosen = item
        loss_value, clipped_fc1, clipped_fc2 = selected_terms(chosen, moment[..., :channels], moment[..., channels:], vae_eps, mirror, crop_at, steps_in, noise, weights)
        return ((running[0] + loss_value, running[1] + clipped_fc1, running[2] + clipped_fc2), None)
    start_state = (jnp.zeros((), jnp.float32), jnp.zeros(w_fc1.shape, jnp.float32), jnp.zeros(w_fc1.shape, jnp.float32))
    totals, ignored = lax.scan(accumulate, start_state, inputs)
    update_fc1 = (totals[1] + noise_weight * noise_fc1) / SELECTED
    update_fc2 = (totals[2] + noise_weight * noise_fc2) / SELECTED
    return (update_fc1, update_fc2, totals[0] / SELECTED, latent_moments)
```

```python
from functools import partial
import math

import numpy as np

import jax
import jax.numpy as jnp
from jax import lax
from jax.experimental import pallas as pl
from jax.experimental.pallas import tpu as pltpu
from jax.sharding import PartitionSpec as P

TSTEPS = 1000
CORES = 2

clip_offset = 1e-05
noise_weight = 16.0
norm_epsilon = 1e-06

LINK = jnp.bfloat16
HIGHEST = lax.Precision.HIGHEST
F32 = jnp.float32
BF16 = jnp.bfloat16
GELU_C = math.sqrt(2.0 / math.pi)
GELU_A = 0.044715


def noise_tables(horizon):
    beta = np.linspace(0.0001, 0.02, horizon, dtype=np.float32)
    alpha_bar = np.cumprod(np.float32(1.0) - beta, dtype=np.float32)
    return np.stack([np.sqrt(alpha_bar), np.sqrt(np.float32(1.0) - alpha_bar)])


def position_table(side_cells, width):
    quarter = width // 4
    frequency = np.float32(1.0) / np.power(
        np.float32(10000.0), np.arange(quarter, dtype=np.float32) / np.float32(quarter)
    )
    angles = np.arange(side_cells, dtype=np.float32)[:, None] * frequency[None, :]
    line = np.concatenate([np.sin(angles), np.cos(angles)], axis=1).astype(np.float32)
    return np.concatenate(
        [np.repeat(line, side_cells, axis=0), np.tile(line, (side_cells, 1))], axis=1
    )


def time_features(steps_in, width):
    half_width = width // 2
    rates = jnp.exp(-math.log(10000.0) * jnp.arange(half_width, dtype=F32) / half_width)
    phases = steps_in.astype(F32)[:, None] * rates[None, :]
    return jnp.concatenate([jnp.cos(phases), jnp.sin(phases)], axis=1)


def iota(shape, axis):
    return lax.broadcasted_iota(jnp.int32, shape, axis)


def one_hot(condition, dtype):
    return jnp.where(condition, 1.0, 0.0).astype(dtype)


def conv_kernel(rows, side, feat_ref, weight_ref, out_ref, wide_ref):
    images = out_ref.shape[0]
    channels = feat_ref.shape[2]
    outs = weight_ref.shape[2]
    lanes = side * outs
    spread = one_hot(iota((outs, lanes), 1) % outs == iota((outs, lanes), 0), BF16)
    for tap in range(9):
        wide_ref[:, tap * lanes : (tap + 1) * lanes] = jnp.dot(
            weight_ref[tap], spread, preferred_element_type=F32
        ).astype(BF16)
    offset = iota((rows * side, lanes), 1) // outs - iota((rows * side, lanes), 0) % side

    def image(s, carry):
        block = feat_ref[pl.ds(s * rows, rows)].reshape(rows * side, channels)
        out_ref[s] = jnp.zeros(out_ref.shape[1:], F32)
        for row_tap in range(3):
            first = 3 * row_tap * lanes
            products = jnp.dot(
                block, wide_ref[:, first : first + 3 * lanes], preferred_element_type=F32
            )
            placed = jnp.zeros((rows * side, lanes), F32)
            for col_tap in range(3):
                placed = jnp.where(
                    offset == 1 - col_tap,
                    products[:, col_tap * lanes : (col_tap + 1) * lanes],
                    placed,
                )
            line = jnp.sum(placed.reshape(rows, side, lanes), axis=1)
            start = 2 - row_tap
            out_ref[s, start : start + rows, :] += line
        return carry

    lax.fori_loop(0, images, image, 0)


def local_conv(features, conv_weight):
    images, rows, side, channels = features.shape
    outs = conv_weight.shape[3]
    lanes = side * outs
    padded = -(-(rows + 2) // 8) * 8
    return pl.pallas_call(
        partial(conv_kernel, rows, side),
        out_shape=jax.ShapeDtypeStruct((images, padded, lanes), F32),
        in_specs=[pl.BlockSpec(memory_space=pltpu.VMEM)] * 2,
        out_specs=pl.BlockSpec(memory_space=pltpu.VMEM),
        scratch_shapes=[pltpu.VMEM((channels, 9 * lanes), BF16)],
        compiler_params=pltpu.CompilerParams(vmem_limit_bytes=24 << 20),
        cost_estimate=pl.CostEstimate(
            flops=2 * images * rows * lanes * channels * 9,
            bytes_accessed=features.size * 2,
            transcendentals=0,
        ),
        name="local_conv",
    )(features.reshape(images * rows, side, channels), conv_weight.reshape(9, channels, outs))


def row_mean(values):
    return jnp.sum(values, axis=-1, keepdims=True) * (1.0 / values.shape[-1])


def example_kernel(
    rows,
    blocks,
    flags_ref,
    flips_ref,
    crops_ref,
    steps_ref,
    table_ref,
    parts_ref,
    vae_ref,
    noise_ref,
    stamp_ref,
    w_patch_ref,
    w_time_ref,
    w_ada_ref,
    w_final_ref,
    position_ref,
    *rest,
):
    own_fc1, own_fc2 = rest[0], rest[1]
    mine = rest[2 : 2 + blocks - 1]
    theirs = rest[1 + blocks : 2 * blocks]
    outs = rest[2 * blocks :]
    moments_ref, loss_ref = outs[0], outs[1]
    keep_refs = outs[2 : 2 + blocks]
    send_refs = outs[2 + blocks : 2 + 2 * blocks]
    (
        weight_ref,
        mod_ref,
        hidden_ref,
        slope_ref,
        pre_ref,
        branch_ref,
        grad_ref,
        latent_ref,
        modulation_ref,
        patch_ref,
        final_ref,
    ) = outs[2 + 2 * blocks :]

    sources = parts_ref.shape[0]
    lanes = parts_ref.shape[2]
    side = sources * rows
    channels = vae_ref.shape[1] // side
    cells = side * channels
    views = noise_ref.shape[0] * 2 // side
    half = side // 2
    per_view = half * half
    width = w_patch_ref.shape[1]
    piece = own_fc1.shape[1]
    total = piece * blocks
    entries = views * per_view * 4 * channels
    parity = flags_ref[1]

    for source in range(sources):
        moments_ref[source * rows : (source + 1) * rows, :] = parts_ref[source, 1 : rows + 1, :]
    for source in range(sources):
        if source > 0:
            moments_ref[source * rows : source * rows + 1, :] += parts_ref[
                source - 1, rows + 1 : rows + 2, :
            ]
        if source < sources - 1:
            last = (source + 1) * rows - 1
            moments_ref[last : last + 1, :] += parts_ref[source + 1, 0:1, :]

    @pl.when(flags_ref[0] != 1)
    def _():
        loss_ref[...] = jnp.zeros_like(loss_ref)
        for k in range(blocks):
            keep_refs[k][...] = jnp.zeros_like(keep_refs[k])
            send_refs[k][...] = jnp.zeros_like(send_refs[k])

    @pl.when(flags_ref[0] == 1)
    def _():
        weight_ref[0, 0] = own_fc1[...]
        weight_ref[1, 0] = own_fc2[...]
        for k in range(1, blocks):
            weight_ref[parity, k] = mine[k - 1][...]
            weight_ref[1 - parity, k] = theirs[k - 1][...]

        moments = moments_ref[...]
        into, outof = iota((lanes, cells), 0), iota((lanes, cells), 1)
        cell = outof // channels * (2 * channels) + outof % channels
        mean_part = jnp.dot(moments, one_hot(into == cell, F32), precision=HIGHEST)
        logvar = jnp.dot(moments, one_hot(into == cell + channels, F32), precision=HIGHEST)
        latent_ref[...] = mean_part + jnp.exp(0.5 * logvar) * vae_ref[...]

        conditioning = jnp.dot(stamp_ref[...], w_time_ref[...], preferred_element_type=F32)
        conditioning = conditioning * (1.0 / (1.0 + jnp.exp(-conditioning)))
        modulation_ref[...] = jnp.dot(
            conditioning.astype(BF16), w_ada_ref[...], preferred_element_type=F32
        )

        short = 2 * channels
        wide = 2 * cells
        lane, entry = iota((wide, 2 * short), 0), iota((wide, 2 * short), 1)
        spread = one_hot(lane // cells * short + lane % short == entry, BF16)
        patch_ref[...] = jnp.dot(
            spread, w_patch_ref[...], preferred_element_type=F32
        ).astype(BF16)
        final_ref[...] = lax.dot_general(
            w_final_ref[...], spread, (((1,), (1,)), ((), ())), preferred_element_type=F32
        ).astype(BF16)

        in_patch = iota((per_view, wide), 1) % cells // short == iota((per_view, wide), 0) % half

        def view(a, loss_sum):
            keep_part = table_ref[0, steps_ref[a]]
            blend_part = table_ref[1, steps_ref[a]]
            flip = flips_ref[a]
            row_at, col_at = crops_ref[2 * a], crops_ref[2 * a + 1]
            source, target_lane = iota((cells, cells), 0), iota((cells, cells), 1)
            column = target_lane // channels + (col_at - 2)
            valid = (column >= 0) & (column < side)
            column = jnp.where(flip == 1, side - 1 - column, column)
            pick_col = one_hot(
                valid & (source == column * channels + target_lane % channels), F32
            )
            target_row, source_row = iota((side, side), 0), iota((side, side), 1)
            wanted = target_row % half * 2 + target_row // half + (row_at - 2)
            pick_row = one_hot(source_row == wanted, F32)
            moved = jnp.dot(latent_ref[...], pick_col, precision=HIGHEST)
            moved = jnp.dot(pick_row, moved, precision=HIGHEST)
            moved = jnp.concatenate([moved[:half], moved[half:]], axis=1)
            noise = noise_ref[pl.ds(a * half, half), :]
            noised = keep_part * moved + blend_part * noise

            def over_patches(values):
                return jnp.broadcast_to(values[:, None, :], (half, half, wide)).reshape(
                    per_view, wide
                )

            patches = jnp.where(in_patch, over_patches(noised), 0.0).astype(BF16)
            tokens = jnp.dot(patches, patch_ref[...], preferred_element_type=F32)
            tokens = tokens + position_ref[...]
            shift = modulation_ref[pl.ds(a, 1), 0:width]
            scale = modulation_ref[pl.ds(a, 1), width : 2 * width]
            gate = modulation_ref[pl.ds(a, 1), 2 * width : 3 * width]

            center = tokens - row_mean(tokens)
            variance = row_mean(center * center)
            normed = center * lax.rsqrt(variance + norm_epsilon)
            modulated = (normed * (1.0 + scale) + shift).astype(BF16)
            here = pl.ds(a * per_view, per_view)
            mod_ref[here, :] = modulated

            branch = jnp.zeros((per_view, width), F32)
            for k in range(blocks):
                columns = slice(k * piece, (k + 1) * piece)
                x = jnp.dot(modulated, weight_ref[0, k], preferred_element_type=F32)
                square = x * x
                tanh = jnp.tanh(x * (square * (GELU_C * GELU_A) + GELU_C))
                cdf = 0.5 * tanh + 0.5
                hidden = x * cdf
                slope_ref[:, columns] = cdf + (hidden * (1.0 - cdf)) * (
                    square * (6.0 * GELU_C * GELU_A) + 2.0 * GELU_C
                )
                hidden = hidden.astype(BF16)
                hidden_ref[here, columns] = hidden
                branch = branch + lax.dot_general(
                    hidden, weight_ref[1, k], (((1,), (1,)), ((), ())), preferred_element_type=F32
                )
            mixed = tokens + gate * branch

            center = mixed - row_mean(mixed)
            variance = row_mean(center * center)
            inverse = lax.rsqrt(variance + norm_epsilon)
            normed = center * inverse
            predicted = jnp.dot(normed.astype(BF16), final_ref[...], preferred_element_type=F32)
            residue = jnp.where(in_patch, predicted - over_patches(noise), 0.0)
            loss_sum = loss_sum + residue * residue
            grad_pred = (residue * (2.0 / entries)).astype(BF16)
            grad_normed = lax.dot_general(
                grad_pred, final_ref[...], (((1,), (1,)), ((), ())), preferred_element_type=F32
            )
            grad_mixed = inverse * (
                grad_normed - row_mean(grad_normed) - normed * row_mean(grad_normed * normed)
            )
            grad_branch = (gate * grad_mixed).astype(BF16)
            branch_ref[here, :] = grad_branch
            for k in range(blocks):
                columns = slice(k * piece, (k + 1) * piece)
                grad_hidden = jnp.dot(
                    grad_branch, weight_ref[1, k], preferred_element_type=F32
                )
                pre_ref[here, columns] = (slope_ref[:, columns] * grad_hidden).astype(BF16)
            return loss_sum

        loss_sum = lax.fori_loop(0, views, view, jnp.zeros((per_view, wide), F32))
        loss_ref[...] = jnp.broadcast_to(
            jnp.sum(loss_sum, keepdims=True) * (1.0 / entries), loss_ref.shape
        )

        modulated_t = mod_ref[...].T
        branch_t = branch_ref[...].T
        squares = jnp.zeros((1, piece), F32)
        for k in range(blocks):
            columns = slice(k * piece, (k + 1) * piece)
            grad = jnp.dot(modulated_t, pre_ref[:, columns], preferred_element_type=F32)
            grad_ref[0, k] = grad
            squares = squares + jnp.sum(grad * grad, axis=0, keepdims=True)
            grad = jnp.dot(branch_t, hidden_ref[:, columns], preferred_element_type=F32)
            grad_ref[1, k] = grad
            squares = squares + jnp.sum(grad * grad, axis=0, keepdims=True)
        root_mean = jnp.sqrt(jnp.sum(squares, keepdims=True) / (2 * width * total))
        factor = 1.0 / (root_mean + clip_offset)
        for k in range(blocks):
            keep_refs[k][...] = grad_ref[parity, k] * factor
            send_refs[k][...] = (grad_ref[1 - parity, k] * factor).astype(send_refs[k].dtype)


def example_call(scalars, arrays, own, mine, theirs, rows):
    blocks = len(mine) + 1
    parts, vae, noise, stamp, w_patch = arrays[:5]
    lanes = parts.shape[2]
    side = parts.shape[0] * rows
    width = w_patch.shape[1]
    piece = own[0].shape[1]
    views = noise.shape[0] * 2 // side
    tokens = views * side * side // 4
    cells = vae.shape[1]
    vae_lines = vae
    vmem = pl.BlockSpec(memory_space=pltpu.VMEM)
    smem = pl.BlockSpec(memory_space=pltpu.SMEM)
    inputs = list(arrays) + list(own) + list(mine) + list(theirs)
    out_shape = (
        [jax.ShapeDtypeStruct((side, lanes), F32), jax.ShapeDtypeStruct((8, 128), F32)]
        + [jax.ShapeDtypeStruct((width, piece), F32)] * blocks
        + [jax.ShapeDtypeStruct((width, piece), LINK)] * blocks
    )
    total = piece * blocks
    return pl.pallas_call(
        partial(example_kernel, rows, blocks),
        out_shape=out_shape,
        in_specs=[smem] * len(scalars) + [vmem] * len(inputs),
        out_specs=[vmem] * len(out_shape),
        scratch_shapes=[
            pltpu.VMEM((2, blocks, width, piece), BF16),
            pltpu.VMEM((tokens, width), BF16),
            pltpu.VMEM((tokens, total), BF16),
            pltpu.VMEM((tokens // views, total), F32),
            pltpu.VMEM((tokens, total), BF16),
            pltpu.VMEM((tokens, width), BF16),
            pltpu.VMEM((2, blocks, width, piece), F32),
            pltpu.VMEM((side, cells), F32),
            pltpu.VMEM((stamp.shape[0], 3 * width), F32),
            pltpu.VMEM((2 * cells, width), BF16),
            pltpu.VMEM((width, 2 * cells), BF16),
        ],
        compiler_params=pltpu.CompilerParams(vmem_limit_bytes=48 << 20),
        cost_estimate=pl.CostEstimate(
            flops=10 * tokens * width * total,
            bytes_accessed=20 * width * total,
            transcendentals=tokens * total,
        ),
        name="example",
    )(*scalars, *inputs)


def shift(values, axis, flip):
    count = lax.axis_size(axis)
    return lax.ppermute(values, axis, [(i, i ^ flip) for i in range(count)])


def tree_sum(terms):
    while len(terms) > 1:
        terms = [terms[i] + terms[i + 1] for i in range(0, len(terms), 2)]
    return terms[0]


def per_device(
    features,
    conv_weight,
    vae_noise,
    flips,
    crops,
    tsteps,
    diffusion_noise,
    selected,
    w_patch,
    w_time,
    w_ada,
    w_fc1,
    w_fc2,
    w_final,
    noise_fc1,
    noise_fc2,
):
    groups = lax.axis_size("fsdp")
    sources = lax.axis_size("dp")
    parity = lax.axis_index("dp") % CORES
    even = parity == 0
    local_rows = features[0]
    rows, side = local_rows.shape[1], local_rows.shape[2]
    outs = conv_weight.shape[3]
    channels = outs // 2
    width, piece = w_fc1.shape
    views = flips.shape[2]

    own_kind = jnp.where(even, w_fc1, w_fc2)
    mine = [shift(own_kind, "fsdp", k) for k in range(1, groups)]
    theirs = [shift(block, "dp", 1) for block in mine]

    parts = local_conv(local_rows, conv_weight)
    parts = lax.all_to_all(parts, "dp", split_axis=0, concat_axis=0, tiled=True)

    stamp = time_features(tsteps[0, 0], w_time.shape[0]).astype(BF16)
    stamp = jnp.pad(stamp, ((0, 16 - views), (0, 0)))
    flags = jnp.stack([selected[0, 0], parity.astype(jnp.int32)])
    scalars = [
        flags,
        flips[0, 0],
        crops[0, 0].reshape(2 * views),
        tsteps[0, 0],
        jnp.asarray(noise_tables(TSTEPS)),
    ]
    arrays = [
        parts,
        vae_noise.reshape(side, side * channels),
        diffusion_noise.reshape(views * side // 2, 2 * side * channels),
        stamp,
        w_patch,
        w_time,
        w_ada,
        w_final,
        jnp.asarray(position_table(side // 2, width)),
    ]
    own = (w_fc1, w_fc2)
    blocked = piece % 128 == 0
    if not blocked:
        joined = jnp.concatenate([own_kind] + mine, axis=1)
        other = jnp.concatenate([jnp.where(even, w_fc2, w_fc1)] + theirs, axis=1)
        own = (jnp.where(even, joined, other), jnp.where(even, other, joined))
        mine, theirs = [], []
    moments, loss, *grads = example_call(scalars, arrays, own, mine, theirs, rows)
    keep, send = grads[: len(grads) // 2], grads[len(grads) // 2 :]
    if not blocked:
        keep = jnp.split(keep[0], groups, axis=1)
        send = jnp.split(send[0], groups, axis=1)

    loss = loss + shift(loss, "dp", 1)
    pair = [None] * groups
    for k in list(range(groups - 1, -1, -1)):
        pair[k] = keep[k] + shift(send[k], "dp", 1).astype(F32)
    owned = [pair[0]]
    losses = [loss]
    for k in range(1, groups):
        owned.append(shift(pair[k].astype(LINK), "fsdp", k).astype(F32))
        losses.append(shift(loss, "fsdp", k))
    owned = tree_sum(owned)
    loss = tree_sum(losses)
    low = owned.astype(LINK)
    sums = [low.astype(F32)]
    losses = [loss]
    for k in range(1, sources // CORES):
        sums.append(shift(low, "dp", CORES * k).astype(F32))
        losses.append(shift(loss, "dp", CORES * k))
    summed = tree_sum(sums)
    loss_all = tree_sum(losses)[0, 0]
    partner = shift(summed, "dp", 1)

    selected_count = selected.shape[0] * sources * groups // 2
    sum_fc1 = jnp.where(even, summed, partner)
    sum_fc2 = jnp.where(even, partner, summed)
    update_fc1 = (sum_fc1 + noise_weight * noise_fc1) / selected_count
    update_fc2 = (sum_fc2 + noise_weight * noise_fc2) / selected_count
    latent_moments = moments.reshape(1, 1, side * side * outs)
    return (update_fc1, update_fc2, loss_all / selected_count, latent_moments)


def solution(mesh):
    in_specs = (
        P("fsdp", None, "dp", None, None),
        P(),
        P("dp", "fsdp", None),
        P("dp", "fsdp", None),
        P("dp", "fsdp", None, None),
        P("dp", "fsdp", None),
        P("dp", "fsdp", None, None),
        P("dp", "fsdp"),
        P(),
        P(),
        P(),
        P(None, "fsdp"),
        P(None, "fsdp"),
        P(),
        P(None, "fsdp"),
        P(None, "fsdp"),
    )
    out_specs = (P(None, "fsdp"), P(None, "fsdp"), P(), P("dp", "fsdp", None))
    return jax.shard_map(
        per_device, mesh=mesh, in_specs=in_specs, out_specs=out_specs, check_vma=False
    )
```

```python
from functools import partial
import math

import numpy as np

import jax
import jax.numpy as jnp
from jax import lax
from jax.experimental import pallas as pl
from jax.experimental.pallas import tpu as pltpu
from jax.sharding import PartitionSpec as P


TSTEPS = 1000
CORES = 2

clip_offset = 1e-05
noise_weight = 16.0
norm_epsilon = 1e-06

LINK = jnp.float16
LINK_EXPONENT, LINK_MANTISSA = jnp.finfo(LINK).nexp, jnp.finfo(LINK).nmant
HIGHEST = lax.Precision.HIGHEST
F32 = jnp.float32
BF16 = jnp.bfloat16
GELU_C = math.sqrt(2.0 / math.pi)
GELU_A = 0.044715


def noise_tables(horizon):
    beta = np.linspace(0.0001, 0.02, horizon, dtype=np.float32)
    alpha_bar = np.cumprod(np.float32(1.0) - beta, dtype=np.float32)
    return np.stack([np.sqrt(alpha_bar), np.sqrt(np.float32(1.0) - alpha_bar)])


def position_table(side_cells, width):
    quarter = width // 4
    frequency = np.float32(1.0) / np.power(
        np.float32(10000.0), np.arange(quarter, dtype=np.float32) / np.float32(quarter)
    )
    angles = np.arange(side_cells, dtype=np.float32)[:, None] * frequency[None, :]
    line = np.concatenate([np.sin(angles), np.cos(angles)], axis=1).astype(np.float32)
    blank = np.zeros_like(line)
    return np.stack(
        [np.concatenate([line, blank], axis=1), np.concatenate([blank, line], axis=1)]
    )


def constants(side_cells, width, features):
    half = features // 2
    rates = np.exp(-math.log(10000.0) * np.arange(half, dtype=np.float32) / np.float32(half))
    lines = position_table(side_cells, width)
    rates = np.pad(rates.astype(np.float32), (0, width - half))
    return np.concatenate([lines, np.broadcast_to(rates, lines[:1].shape)]).astype(np.float32)


def iota(shape, axis):
    return lax.broadcasted_iota(jnp.int32, shape, axis)


def one_hot(condition, dtype):
    return jnp.where(condition, 1.0, 0.0).astype(dtype)


def split_float(values):
    high = values.astype(BF16)
    rest = values - high.astype(F32)
    middle = rest.astype(BF16)
    return high, middle, (rest - middle.astype(F32)).astype(BF16)


def conv_kernel(rows, side, outs, feat_ref, weight_ref, out_ref):
    images = out_ref.shape[0]
    cells, channels = feat_ref.shape
    lanes = side * outs
    taps = 128
    weights = jnp.concatenate(
        [weight_ref[...], jnp.zeros((taps - 9 * outs, channels), BF16)], axis=0
    )
    products = lax.dot_general(
        feat_ref[...], weights, (((1,), (1,)), ((), ())), preferred_element_type=F32
    )
    zero_row = jnp.zeros((1, taps), F32)
    before = jnp.concatenate([zero_row, products[: cells - 1]], axis=0)
    after = jnp.concatenate([products[1:], zero_row], axis=0)
    column = iota((cells, taps), 0) % side
    tap = iota((cells, taps), 1) // outs % 3
    chosen = jnp.where(
        tap == 1,
        products,
        jnp.where(
            tap == 0,
            jnp.where(column == 0, 0.0, before),
            jnp.where(column == side - 1, 0.0, after),
        ),
    )
    source, target = iota((taps, 3 * lanes), 0), iota((taps, 3 * lanes), 1)
    wanted = (source // (3 * outs) == target // lanes) & (source % outs == target % outs)
    spread = one_hot(wanted & (source < 9 * outs), BF16)
    wide = jnp.zeros((cells, 3 * lanes), F32)
    for part in split_float(chosen):
        wide = wide + jnp.dot(part, spread, preferred_element_type=F32)
    own = iota((cells, lanes), 1) // outs == iota((cells, lanes), 0) % side
    out_ref[...] = jnp.zeros(out_ref.shape, F32)
    for row_tap in range(3):
        placed = jnp.where(own, wide[:, row_tap * lanes : (row_tap + 1) * lanes], 0.0)
        line = jnp.sum(placed.reshape(images * rows, side, lanes), axis=1)
        line = line.reshape(images, rows, lanes)
        start = 2 - row_tap
        for s in range(images):
            out_ref[s, start : start + rows, :] += line[s]


def local_conv(features, conv_weight):
    images, rows, side, channels = features.shape
    outs = conv_weight.shape[3]
    lanes = side * outs
    padded = -(-(rows + 2) // 8) * 8
    weight = conv_weight.transpose(0, 1, 3, 2).reshape(9 * outs, channels)
    return pl.pallas_call(
        partial(conv_kernel, rows, side, outs),
        out_shape=jax.ShapeDtypeStruct((images, padded, lanes), F32),
        in_specs=[pl.BlockSpec(memory_space=pltpu.VMEM)] * 2,
        out_specs=pl.BlockSpec(memory_space=pltpu.VMEM),
        compiler_params=pltpu.CompilerParams(vmem_limit_bytes=24 << 20),
        cost_estimate=pl.CostEstimate(
            flops=2 * images * rows * lanes * channels * 9,
            bytes_accessed=features.size * 2,
            transcendentals=0,
        ),
        name="local_conv",
    )(features.reshape(images * rows * side, channels), weight)


def row_mean(values):
    return jnp.sum(values, axis=-1, keepdims=True) * (1.0 / values.shape[-1])


def patch_mask(per_view, half, wide, short):
    cells = wide // 2
    return iota((per_view, wide), 1) % cells // short == iota((per_view, wide), 0) % half


def over_patches(values):
    half, wide = values.shape
    return jnp.broadcast_to(values[:, None, :], (half, half, wide)).reshape(half * half, wide)


def prepare_kernel(
    side,
    flips_ref,
    crops_ref,
    steps_ref,
    table_ref,
    constant_hbm,
    noise_hbm,
    w_patch_hbm,
    w_time_hbm,
    w_ada_hbm,
    w_final_hbm,
    modulation_ref,
    patch_ref,
    final_ref,
    place_ref,
    noise_ref,
    column_ref,
    row_ref,
    constant_ref,
    raw_noise_ref,
    w_patch_ref,
    w_time_ref,
    w_ada_ref,
    w_final_ref,
    sems,
):
    views = steps_ref.shape[0]
    half = side // 2
    wide = noise_ref.shape[1]
    cells = wide // 2
    short = cells // half
    channels = short // 2
    width = w_patch_ref.shape[1]
    half_freq = w_time_ref.shape[0] // 2
    sources = (constant_hbm, noise_hbm, w_patch_hbm, w_time_hbm, w_ada_hbm, w_final_hbm)
    targets = (constant_ref, raw_noise_ref, w_patch_ref, w_time_ref, w_ada_ref, w_final_ref)
    copies = [
        pltpu.make_async_copy(source, target, sems.at[n])
        for n, (source, target) in enumerate(zip(sources, targets))
    ]
    for copy in copies:
        copy.start()

    source, target = iota((cells, cells), 0), iota((cells, cells), 1)
    target_row, source_row = iota((side, side), 0), iota((side, side), 1)
    for a in range(views):
        column = target // channels + (crops_ref[1, a] - 2)
        valid = (column >= 0) & (column < side)
        column = jnp.where(flips_ref[a] == 1, side - 1 - column, column)
        column_ref[a] = one_hot(
            valid & (source == column * channels + target % channels), F32
        )
        wanted = target_row % half * 2 + target_row // half + (crops_ref[0, a] - 2)
        row_ref[a] = one_hot(source_row == wanted, F32)

    for copy in copies:
        copy.wait()
    steps = jnp.zeros((modulation_ref.shape[0], half_freq), F32)
    for a in range(views):
        steps = jnp.where(iota(steps.shape, 0) == a, steps_ref[a].astype(F32), steps)
    phases = steps * constant_ref[2, 0:1, :half_freq]
    stamp = jnp.concatenate([jnp.cos(phases), jnp.sin(phases)], axis=1).astype(BF16)
    conditioning = jnp.dot(stamp, w_time_ref[...], preferred_element_type=F32)
    conditioning = conditioning * (1.0 / (1.0 + jnp.exp(-conditioning)))
    modulation_ref[...] = jnp.dot(
        conditioning.astype(BF16), w_ada_ref[...], preferred_element_type=F32
    )
    lane, entry = iota((wide, 2 * short), 0), iota((wide, 2 * short), 1)
    spread = one_hot(lane // cells * short + lane % short == entry, BF16)
    patch_ref[...] = jnp.dot(spread, w_patch_ref[...], preferred_element_type=F32).astype(BF16)
    final_ref[...] = jnp.dot(spread, w_final_ref[...], preferred_element_type=F32).astype(BF16)
    place_ref[...] = (
        jnp.broadcast_to(constant_ref[0][:, None, :], (half, half, width))
        + jnp.broadcast_to(constant_ref[1][None, :, :], (half, half, width))
    ).reshape(half * half, width)
    for a in range(views):
        for line in range(half):
            n = a * half + line
            noise_ref[n : n + 1, :] = raw_noise_ref[a : a + 1, line * wide : (line + 1) * wide]


def token_kernel(
    rows,
    chosen_ref,
    steps_ref,
    table_ref,
    parts_ref,
    vae_ref,
    modulation_ref,
    patch_ref,
    place_ref,
    noise_ref,
    column_ref,
    row_ref,
    moments_ref,
    token_ref,
    mod_ref,
    latent_ref,
):
    sources = parts_ref.shape[0]
    lanes = parts_ref.shape[2]
    side = sources * rows
    channels = vae_ref.shape[1] // side
    cells = side * channels
    views = steps_ref.shape[0]
    half = side // 2
    per_view = half * half
    width = patch_ref.shape[1]
    short = 2 * channels
    wide = 2 * cells

    for source in range(sources):
        moments_ref[source * rows : (source + 1) * rows, :] = parts_ref[source, 1 : rows + 1, :]
    for source in range(sources):
        if source > 0:
            moments_ref[source * rows : source * rows + 1, :] += parts_ref[
                source - 1, rows + 1 : rows + 2, :
            ]
        if source < sources - 1:
            last = (source + 1) * rows - 1
            moments_ref[last : last + 1, :] += parts_ref[source + 1, 0:1, :]

    @pl.when(chosen_ref[0, 0] == 1)
    def _():
        moments = moments_ref[...]
        into, outof = iota((lanes, cells), 0), iota((lanes, cells), 1)
        cell = outof // channels * (2 * channels) + outof % channels
        mean_part = jnp.dot(moments, one_hot(into == cell, F32), precision=HIGHEST)
        logvar = jnp.dot(moments, one_hot(into == cell + channels, F32), precision=HIGHEST)
        latent_ref[...] = mean_part + jnp.exp(0.5 * logvar) * vae_ref[...]
        in_patch = patch_mask(per_view, half, wide, short)

        for a in range(views):
            keep_part = table_ref[0, steps_ref[a]]
            blend_part = table_ref[1, steps_ref[a]]
            moved = jnp.dot(latent_ref[...], column_ref[a], precision=HIGHEST)
            moved = jnp.dot(row_ref[a], moved, precision=HIGHEST)
            moved = jnp.concatenate([moved[:half], moved[half:]], axis=1)
            noised = keep_part * moved + blend_part * noise_ref[a * half : (a + 1) * half, :]
            patches = jnp.where(in_patch, over_patches(noised), 0.0).astype(BF16)
            tokens = jnp.dot(patches, patch_ref[...], preferred_element_type=F32)
            tokens = tokens + place_ref[...]
            shift_row = modulation_ref[a : a + 1, 0:width]
            scale_row = modulation_ref[a : a + 1, width : 2 * width]
            center = tokens - row_mean(tokens)
            variance = row_mean(center * center)
            normed = center * lax.rsqrt(variance + norm_epsilon)
            here = slice(a * per_view, (a + 1) * per_view)
            token_ref[here, :] = tokens
            mod_ref[here, :] = (normed * (1.0 + scale_row) + shift_row).astype(BF16)


def grad_kernel(blocks, views, chosen_ref, parity_ref, noise_ref, token_ref, mod_ref, modulation_ref, final_ref, *rest):
    own_fc1, own_fc2 = rest[0], rest[1]
    mine = rest[2 : 2 + blocks - 1]
    theirs = rest[1 + blocks : 2 * blocks]
    outs = rest[2 * blocks :]
    loss_ref = outs[0]
    keep_refs = outs[1 : 1 + blocks]
    send_refs = outs[1 + blocks : 1 + 2 * blocks]
    weight_ref, hidden_ref, slope_ref, pre_ref, branch_ref, grad_ref = outs[1 + 2 * blocks :]

    tokens_count, width = token_ref.shape
    wide = noise_ref.shape[1]
    half = noise_ref.shape[0] // views
    per_view = half * half
    short = wide // 2 // half
    piece = own_fc1.shape[1]
    total = piece * blocks
    entries = tokens_count * 2 * short
    parity = parity_ref[0]

    @pl.when(chosen_ref[0, 0] != 1)
    def _():
        loss_ref[...] = jnp.zeros_like(loss_ref)
        for k in range(blocks):
            keep_refs[k][...] = jnp.zeros_like(keep_refs[k])
            send_refs[k][...] = jnp.zeros_like(send_refs[k])

    @pl.when(chosen_ref[0, 0] == 1)
    def _():
        weight_ref[0, 0] = own_fc1[...]
        weight_ref[1, 0] = own_fc2[...]
        for k in range(1, blocks):
            weight_ref[parity, k] = mine[k - 1][...]
            weight_ref[1 - parity, k] = theirs[k - 1][...]
        in_patch = patch_mask(per_view, half, wide, short)

        def columns(k):
            return slice(k * piece, (k + 1) * piece)

        def view(a, loss_sum):
            here = pl.ds(a * per_view, per_view)
            gate = modulation_ref[pl.ds(a, 1), 2 * width : 3 * width]
            modulated = mod_ref[here, :]
            branch = jnp.zeros((per_view, width), F32)
            for k in range(blocks):
                x = jnp.dot(modulated, weight_ref[0, k], preferred_element_type=F32)
                square = x * x
                tanh = jnp.tanh(x * (square * (GELU_C * GELU_A) + GELU_C))
                cdf = 0.5 * tanh + 0.5
                hidden = x * cdf
                slope_ref[:, columns(k)] = cdf + (hidden * (1.0 - cdf)) * (
                    square * (6.0 * GELU_C * GELU_A) + 2.0 * GELU_C
                )
                hidden = hidden.astype(BF16)
                hidden_ref[here, columns(k)] = hidden
                branch = branch + lax.dot_general(
                    hidden, weight_ref[1, k], (((1,), (1,)), ((), ())), preferred_element_type=F32
                )
            mixed = token_ref[here, :] + gate * branch
            center = mixed - row_mean(mixed)
            variance = row_mean(center * center)
            inverse = lax.rsqrt(variance + norm_epsilon)
            normed = center * inverse
            predicted = lax.dot_general(
                normed.astype(BF16), final_ref[...], (((1,), (1,)), ((), ())),
                preferred_element_type=F32,
            )
            noise = noise_ref[pl.ds(a * half, half), :]
            residue = jnp.where(in_patch, predicted - over_patches(noise), 0.0)
            loss_sum = loss_sum + jnp.sum(residue * residue, axis=0, keepdims=True)
            grad_pred = (residue * (2.0 / entries)).astype(BF16)
            grad_normed = jnp.dot(grad_pred, final_ref[...], preferred_element_type=F32)
            grad_mixed = inverse * (
                grad_normed - row_mean(grad_normed) - normed * row_mean(grad_normed * normed)
            )
            grad_branch = (gate * grad_mixed).astype(BF16)
            branch_ref[here, :] = grad_branch
            for k in range(blocks):
                grad_hidden = jnp.dot(
                    grad_branch, weight_ref[1, k], preferred_element_type=F32
                )
                pre_ref[here, columns(k)] = (slope_ref[:, columns(k)] * grad_hidden).astype(BF16)
            return loss_sum

        loss_sum = lax.fori_loop(0, views, view, jnp.zeros((1, wide), F32))
        loss_ref[...] = jnp.broadcast_to(
            jnp.sum(loss_sum, keepdims=True) * (1.0 / entries), loss_ref.shape
        )

        modulated_t = mod_ref[...].T
        branch_t = branch_ref[...].T
        squares = jnp.zeros((1, piece), F32)
        for k in range(blocks):
            grad = jnp.dot(modulated_t, pre_ref[:, columns(k)], preferred_element_type=F32)
            grad_ref[0, k] = grad
            squares = squares + jnp.sum(grad * grad, axis=0, keepdims=True)
            grad = jnp.dot(branch_t, hidden_ref[:, columns(k)], preferred_element_type=F32)
            grad_ref[1, k] = grad
            squares = squares + jnp.sum(grad * grad, axis=0, keepdims=True)
        root_mean = jnp.sqrt(jnp.sum(squares, keepdims=True) / (2 * width * total))
        factor = 1.0 / (root_mean + clip_offset)
        for k in range(blocks):
            keep_refs[k][...] = grad_ref[parity, k] * factor
            send_refs[k][...] = grad_ref[1 - parity, k] * factor


VMEM = pl.BlockSpec(memory_space=pltpu.VMEM)
SMEM = pl.BlockSpec(memory_space=pltpu.SMEM)
HBM = pl.BlockSpec(memory_space=pltpu.HBM)


def prepare_call(scalars, constant, noise, weights, side):
    views, flat = noise.shape
    half = side // 2
    wide = flat // half
    cells = wide // 2
    width = weights[0].shape[1]
    inputs = [constant, noise, *weights]
    out_shape = [
        jax.ShapeDtypeStruct((16, 3 * width), F32),
        jax.ShapeDtypeStruct((wide, width), BF16),
        jax.ShapeDtypeStruct((wide, width), BF16),
        jax.ShapeDtypeStruct((half * half, width), F32),
        jax.ShapeDtypeStruct((views * half, wide), F32),
        jax.ShapeDtypeStruct((views, cells, cells), F32),
        jax.ShapeDtypeStruct((views, side, side), F32),
    ]
    return pl.pallas_call(
        partial(prepare_kernel, side),
        out_shape=out_shape,
        in_specs=[SMEM] * len(scalars) + [HBM] * len(inputs),
        out_specs=[VMEM] * len(out_shape),
        scratch_shapes=[pltpu.VMEM(v.shape, v.dtype) for v in inputs]
        + [pltpu.SemaphoreType.DMA((len(inputs),))],
        compiler_params=pltpu.CompilerParams(vmem_limit_bytes=52 << 20),
        cost_estimate=pl.CostEstimate(
            flops=1 << 27, bytes_accessed=1 << 21, transcendentals=0
        ),
        name="prepare",
    )(*scalars, *inputs)


def token_call(scalars, arrays, rows):
    parts, vae, _, patch, place = arrays[:5]
    lanes = parts.shape[2]
    side = parts.shape[0] * rows
    width = patch.shape[1]
    views = scalars[1].shape[0]
    tokens = views * place.shape[0]
    cells = vae.shape[1]
    out_shape = [
        jax.ShapeDtypeStruct((side, lanes), F32),
        jax.ShapeDtypeStruct((tokens, width), F32),
        jax.ShapeDtypeStruct((tokens, width), BF16),
    ]
    return pl.pallas_call(
        partial(token_kernel, rows),
        out_shape=out_shape,
        in_specs=[SMEM] * len(scalars) + [VMEM] * len(arrays),
        out_specs=[VMEM] * len(out_shape),
        scratch_shapes=[pltpu.VMEM((side, cells), F32)],
        compiler_params=pltpu.CompilerParams(vmem_limit_bytes=20 << 20),
        cost_estimate=pl.CostEstimate(
            flops=4 * tokens * width * cells, bytes_accessed=16 * tokens * width, transcendentals=0
        ),
        name="tokens",
    )(*scalars, *arrays)


def grad_call(chosen, parity, views, arrays, own, mine, theirs):
    blocks = len(mine) + 1
    _, token = arrays[:2]
    tokens, width = token.shape
    per_view = tokens // views
    piece = own[0].shape[1]
    total = piece * blocks
    inputs = list(arrays) + list(own) + list(mine) + list(theirs)
    out_shape = [jax.ShapeDtypeStruct((16, 128), F32)] + [
        jax.ShapeDtypeStruct((width, piece), F32)
    ] * (2 * blocks)
    return pl.pallas_call(
        partial(grad_kernel, blocks, views),
        out_shape=out_shape,
        in_specs=[SMEM] * 2 + [VMEM] * len(inputs),
        out_specs=[VMEM] * len(out_shape),
        scratch_shapes=[
            pltpu.VMEM((2, blocks, width, piece), BF16),
            pltpu.VMEM((tokens, total), BF16),
            pltpu.VMEM((per_view, total), F32),
            pltpu.VMEM((tokens, total), BF16),
            pltpu.VMEM((tokens, width), BF16),
            pltpu.VMEM((2, blocks, width, piece), F32),
        ],
        compiler_params=pltpu.CompilerParams(vmem_limit_bytes=36 << 20),
        cost_estimate=pl.CostEstimate(
            flops=10 * tokens * width * total,
            bytes_accessed=20 * width * total,
            transcendentals=tokens * total,
        ),
        name="grads",
    )(chosen, parity, *inputs)


def shift(values, axis, flip):
    count = lax.axis_size(axis)
    return lax.ppermute(values, axis, [(i, i ^ flip) for i in range(count)])


LOSS_SCALE = 64.0
NEXT = 2.0 ** (LINK_MANTISSA + 1)


def to_link(values):
    return lax.reduce_precision(values, LINK_EXPONENT, LINK_MANTISSA)


def pack_loss(loss):
    high = to_link(loss * (1.0 / LOSS_SCALE))
    rest = (loss * (1.0 / LOSS_SCALE) - high) * NEXT
    middle = to_link(rest)
    low = to_link((rest - middle) * NEXT)
    return jnp.concatenate([high, middle, low], axis=1)


def unpack_loss(packed):
    high, middle, low = jnp.split(packed.astype(F32), 3, axis=1)
    return (high + (middle + low * (1.0 / NEXT)) * (1.0 / NEXT)) * LOSS_SCALE


def per_device(
    features,
    conv_weight,
    vae_noise,
    flips,
    crops,
    tsteps,
    diffusion_noise,
    selected,
    w_patch,
    w_time,
    w_ada,
    w_fc1,
    w_fc2,
    w_final,
    noise_fc1,
    noise_fc2,
):
    groups = lax.axis_size("fsdp")
    sources = lax.axis_size("dp")
    parity = lax.axis_index("dp") % CORES
    even = parity == 0
    local_rows = features[0]
    rows, side = local_rows.shape[1], local_rows.shape[2]
    outs = conv_weight.shape[3]
    channels = outs // 2
    width, piece = w_fc1.shape
    views = flips.shape[2]

    own_kind = jnp.where(even, w_fc1, w_fc2)
    mine = [shift(own_kind, "fsdp", k) for k in range(1, groups)]

    local = local_conv(local_rows, conv_weight)
    parts = lax.all_to_all(local, "dp", split_axis=0, concat_axis=0, tiled=True)
    steps = tsteps[0, 0]
    table = jnp.asarray(noise_tables(TSTEPS))
    constant = jnp.asarray(constants(side // 2, width, w_time.shape[0]))
    modulation, patch, final, place, noise, column, row = prepare_call(
        [flips[0, 0], crops[0, 0].T, steps, table],
        constant,
        diffusion_noise[0, 0],
        lax.optimization_barrier((w_patch, w_time, w_ada, w_final.T, local))[:4],
        side,
    )
    *mine, modulation = lax.optimization_barrier((*mine, modulation))
    theirs = [shift(block, "dp", 1) for block in mine]
    own = (w_fc1, w_fc2)
    blocked = piece % 128 == 0
    if not blocked:
        joined = jnp.concatenate([own_kind] + mine, axis=1)
        other = jnp.concatenate([jnp.where(even, w_fc2, w_fc1)] + theirs, axis=1)
        own = (jnp.where(even, joined, other), jnp.where(even, other, joined))
        mine, theirs = [], []
    moments, tokens, modulated = token_call(
        [selected, steps, table],
        [parts, vae_noise.reshape(side, side * channels)]
        + [modulation, patch, place, noise, column, row],
        rows,
    )
    loss, *grads = grad_call(
        selected,
        parity.astype(jnp.int32).reshape(1),
        views,
        [noise, tokens, modulated, modulation, final],
        own,
        mine,
        theirs,
    )
    keep, send = grads[: len(grads) // 2], grads[len(grads) // 2 :]
    if not blocked:
        keep = jnp.split(keep[0], groups, axis=1)
        send = jnp.split(send[0], groups, axis=1)

    loss = loss[:, : piece // 3]
    received = [shift(block, "dp", 1) for block in send]
    *received, other = lax.optimization_barrier((*received, shift(loss, "dp", 1)))
    pair = [kept + block for kept, block in zip(keep, received)]
    loss = loss + other
    middle = width // 2
    halves = [[block[:middle] for block in pair], [block[middle:] for block in pair]]

    def exchange(moving, axis, flips_of):
        packed = pack_loss(loss)
        moved = [
            jnp.concatenate([moving[0], packed], axis=0).astype(LINK),
            moving[1].astype(LINK),
        ]
        moved = [shift(block, axis, flip) for block, flip in zip(moved, flips_of)]
        first, second = [block.astype(F32) for block in lax.optimization_barrier(moved)]
        size = moving[0].shape[0]
        return (first[:size], second), unpack_loss(packed) + unpack_loss(first[size:])

    bits = [1 << b for b in range(groups.bit_length() - 1)]
    for step in range(len(bits)):
        flips_of = (bits[step], bits[-1 - step])
        gone = [
            [k for k in range(groups) if k & bit and half[k] is not None]
            for half, bit in zip(halves, flips_of)
        ]
        moving = [
            jnp.concatenate([half[k] for k in ks], axis=0) for half, ks in zip(halves, gone)
        ]
        received, loss = exchange(moving, "fsdp", flips_of)
        for half, bit, ks, moved in zip(halves, flips_of, gone, received):
            for n, k in enumerate(ks):
                half[k ^ bit] = half[k ^ bit] + moved[n * middle : (n + 1) * middle]
                half[k] = None
    halves = [half[0] for half in halves]
    chips = sources // CORES
    hops = [(2 << b) - 1 for b in range(chips.bit_length() - 1)]
    for step in range(len(hops)):
        halves = [to_link(half) for half in halves]
        flips_of = (CORES * hops[step], CORES * hops[-1 - step])
        received, loss = exchange(halves, "dp", flips_of)
        halves = [half + moved for half, moved in zip(halves, received)]
    partner = [shift(half, "dp", 1) for half in halves]
    summed = jnp.concatenate(halves, axis=0)
    partner = jnp.concatenate(partner, axis=0)
    loss_all = lax.optimization_barrier(loss)[0, 0]

    selected_count = selected.shape[0] * sources * groups // 2
    sum_fc1 = jnp.where(even, summed, partner)
    sum_fc2 = jnp.where(even, partner, summed)
    update_fc1 = (sum_fc1 + noise_weight * noise_fc1) / selected_count
    update_fc2 = (sum_fc2 + noise_weight * noise_fc2) / selected_count
    latent_moments = moments.reshape(1, 1, side * side * outs)
    return (update_fc1, update_fc2, loss_all / selected_count, latent_moments)


def solution(mesh):
    in_specs = (
        P("fsdp", None, "dp", None, None),
        P(),
        P("dp", "fsdp", None),
        P("dp", "fsdp", None),
        P("dp", "fsdp", None, None),
        P("dp", "fsdp", None),
        P("dp", "fsdp", None, None),
        P("dp", "fsdp"),
        P(),
        P(),
        P(),
        P(None, "fsdp"),
        P(None, "fsdp"),
        P(),
        P(None, "fsdp"),
        P(None, "fsdp"),
    )
    out_specs = (P(None, "fsdp"), P(None, "fsdp"), P(), P("dp", "fsdp", None))
    return jax.shard_map(
        per_device, mesh=mesh, in_specs=in_specs, out_specs=out_specs, check_vma=False
    )
```

```python
from functools import partial
import math

import numpy as np

import jax
import jax.numpy as jnp
from jax import lax
from jax.experimental import pallas as pl
from jax.experimental.pallas import tpu as pltpu
from jax.sharding import PartitionSpec as P


TSTEPS = 1000
CORES = 2

clip_offset = 1e-05
noise_weight = 16.0
norm_epsilon = 1e-06

LINK = jnp.float16
LINK_EXPONENT, LINK_MANTISSA = jnp.finfo(LINK).nexp, jnp.finfo(LINK).nmant
HIGHEST = lax.Precision.HIGHEST
F32 = jnp.float32
BF16 = jnp.bfloat16
GELU_C = math.sqrt(2.0 / math.pi)
GELU_A = 0.044715


def noise_tables(horizon):
    beta = np.linspace(0.0001, 0.02, horizon, dtype=np.float32)
    alpha_bar = np.cumprod(np.float32(1.0) - beta, dtype=np.float32)
    return np.stack([np.sqrt(alpha_bar), np.sqrt(np.float32(1.0) - alpha_bar)])


def position_table(side_cells, width):
    quarter = width // 4
    frequency = np.float32(1.0) / np.power(
        np.float32(10000.0), np.arange(quarter, dtype=np.float32) / np.float32(quarter)
    )
    angles = np.arange(side_cells, dtype=np.float32)[:, None] * frequency[None, :]
    line = np.concatenate([np.sin(angles), np.cos(angles)], axis=1).astype(np.float32)
    blank = np.zeros_like(line)
    return np.stack(
        [np.concatenate([line, blank], axis=1), np.concatenate([blank, line], axis=1)]
    )


def constants(side_cells, width, features):
    half = features // 2
    rates = np.exp(-math.log(10000.0) * np.arange(half, dtype=np.float32) / np.float32(half))
    lines = position_table(side_cells, width)
    rates = np.pad(rates.astype(np.float32), (0, width - half))
    return np.concatenate([lines, np.broadcast_to(rates, lines[:1].shape)]).astype(np.float32)


def iota(shape, axis):
    return lax.broadcasted_iota(jnp.int32, shape, axis)


def one_hot(condition, dtype):
    return jnp.where(condition, 1.0, 0.0).astype(dtype)


def split_float(values):
    high = values.astype(BF16)
    rest = values - high.astype(F32)
    middle = rest.astype(BF16)
    return high, middle, (rest - middle.astype(F32)).astype(BF16)


def conv_kernel(rows, side, outs, feat_ref, weight_ref, out_ref):
    images = out_ref.shape[0]
    cells, channels = feat_ref.shape
    lanes = side * outs
    taps = 128
    weights = jnp.concatenate(
        [weight_ref[...], jnp.zeros((taps - 9 * outs, channels), BF16)], axis=0
    )
    products = lax.dot_general(
        feat_ref[...], weights, (((1,), (1,)), ((), ())), preferred_element_type=F32
    )
    zero_row = jnp.zeros((1, taps), F32)
    before = jnp.concatenate([zero_row, products[: cells - 1]], axis=0)
    after = jnp.concatenate([products[1:], zero_row], axis=0)
    column = iota((cells, taps), 0) % side
    tap = iota((cells, taps), 1) // outs % 3
    chosen = jnp.where(
        tap == 1,
        products,
        jnp.where(
            tap == 0,
            jnp.where(column == 0, 0.0, before),
            jnp.where(column == side - 1, 0.0, after),
        ),
    )
    source, target = iota((taps, 3 * lanes), 0), iota((taps, 3 * lanes), 1)
    wanted = (source // (3 * outs) == target // lanes) & (source % outs == target % outs)
    spread = one_hot(wanted & (source < 9 * outs), BF16)
    wide = jnp.zeros((cells, 3 * lanes), F32)
    for part in split_float(chosen):
        wide = wide + jnp.dot(part, spread, preferred_element_type=F32)
    own = iota((cells, lanes), 1) // outs == iota((cells, lanes), 0) % side
    out_ref[...] = jnp.zeros(out_ref.shape, F32)
    for row_tap in range(3):
        placed = jnp.where(own, wide[:, row_tap * lanes : (row_tap + 1) * lanes], 0.0)
        line = jnp.sum(placed.reshape(images * rows, side, lanes), axis=1)
        line = line.reshape(images, rows, lanes)
        start = 2 - row_tap
        for s in range(images):
            out_ref[s, start : start + rows, :] += line[s]


def local_conv(features, conv_weight):
    images, rows, side, channels = features.shape
    outs = conv_weight.shape[3]
    lanes = side * outs
    padded = -(-(rows + 2) // 8) * 8
    weight = conv_weight.transpose(0, 1, 3, 2).reshape(9 * outs, channels)
    return pl.pallas_call(
        partial(conv_kernel, rows, side, outs),
        out_shape=jax.ShapeDtypeStruct((images, padded, lanes), F32),
        in_specs=[pl.BlockSpec(memory_space=pltpu.VMEM)] * 2,
        out_specs=pl.BlockSpec(memory_space=pltpu.VMEM),
        compiler_params=pltpu.CompilerParams(vmem_limit_bytes=56 << 20),
        cost_estimate=pl.CostEstimate(
            flops=2 * images * rows * lanes * channels * 9,
            bytes_accessed=features.size * 2,
            transcendentals=0,
        ),
        name="local_conv",
    )(features.reshape(images * rows * side, channels), weight)


def row_mean(values):
    return jnp.sum(values, axis=-1, keepdims=True) * (1.0 / values.shape[-1])


def patch_mask(per_view, half, wide, short):
    cells = wide // 2
    return iota((per_view, wide), 1) % cells // short == iota((per_view, wide), 0) % half


def over_patches(values):
    half, wide = values.shape
    return jnp.broadcast_to(values[:, None, :], (half, half, wide)).reshape(half * half, wide)


def prepare_kernel(
    side,
    flips_ref,
    crops_ref,
    steps_ref,
    table_ref,
    constant_hbm,
    noise_hbm,
    w_patch_hbm,
    w_time_hbm,
    w_ada_hbm,
    w_final_hbm,
    modulation_ref,
    patch_ref,
    final_ref,
    place_ref,
    noise_ref,
    column_ref,
    row_ref,
    constant_ref,
    raw_noise_ref,
    w_patch_ref,
    w_time_ref,
    w_ada_ref,
    w_final_ref,
    sems,
):
    views = steps_ref.shape[0]
    half = side // 2
    wide = noise_ref.shape[1]
    cells = wide // 2
    short = cells // half
    channels = short // 2
    width = w_patch_ref.shape[1]
    half_freq = w_time_ref.shape[0] // 2
    sources = (constant_hbm, noise_hbm, w_patch_hbm, w_time_hbm, w_ada_hbm, w_final_hbm)
    targets = (constant_ref, raw_noise_ref, w_patch_ref, w_time_ref, w_ada_ref, w_final_ref)
    copies = [
        pltpu.make_async_copy(source, target, sems.at[n])
        for n, (source, target) in enumerate(zip(sources, targets))
    ]
    for copy in copies:
        copy.start()

    source, target = iota((cells, cells), 0), iota((cells, cells), 1)
    target_row, source_row = iota((side, side), 0), iota((side, side), 1)
    for a in range(views):
        column = target // channels + (crops_ref[1, a] - 2)
        valid = (column >= 0) & (column < side)
        column = jnp.where(flips_ref[a] == 1, side - 1 - column, column)
        column_ref[a] = one_hot(
            valid & (source == column * channels + target % channels), F32
        )
        wanted = target_row % half * 2 + target_row // half + (crops_ref[0, a] - 2)
        row_ref[a] = one_hot(source_row == wanted, F32)

    for copy in copies:
        copy.wait()
    steps = jnp.zeros((modulation_ref.shape[0], half_freq), F32)
    for a in range(views):
        steps = jnp.where(iota(steps.shape, 0) == a, steps_ref[a].astype(F32), steps)
    phases = steps * constant_ref[2, 0:1, :half_freq]
    stamp = jnp.concatenate([jnp.cos(phases), jnp.sin(phases)], axis=1).astype(BF16)
    conditioning = jnp.dot(stamp, w_time_ref[...], preferred_element_type=F32)
    conditioning = conditioning * (1.0 / (1.0 + jnp.exp(-conditioning)))
    modulation_ref[...] = jnp.dot(
        conditioning.astype(BF16), w_ada_ref[...], preferred_element_type=F32
    )
    lane, entry = iota((wide, 2 * short), 0), iota((wide, 2 * short), 1)
    spread = one_hot(lane // cells * short + lane % short == entry, BF16)
    patch_ref[...] = jnp.dot(spread, w_patch_ref[...], preferred_element_type=F32).astype(BF16)
    final_ref[...] = jnp.dot(spread, w_final_ref[...], preferred_element_type=F32).astype(BF16)
    place_ref[...] = (
        jnp.broadcast_to(constant_ref[0][:, None, :], (half, half, width))
        + jnp.broadcast_to(constant_ref[1][None, :, :], (half, half, width))
    ).reshape(half * half, width)
    for a in range(views):
        for line in range(half):
            n = a * half + line
            noise_ref[n : n + 1, :] = raw_noise_ref[a : a + 1, line * wide : (line + 1) * wide]


def token_kernel(
    rows,
    chosen_ref,
    steps_ref,
    table_ref,
    parts_ref,
    vae_ref,
    modulation_ref,
    patch_ref,
    place_ref,
    noise_ref,
    column_ref,
    row_ref,
    moments_ref,
    token_ref,
    mod_ref,
    latent_ref,
):
    sources = parts_ref.shape[0]
    lanes = parts_ref.shape[2]
    side = sources * rows
    channels = vae_ref.shape[1] // side
    cells = side * channels
    views = steps_ref.shape[0]
    half = side // 2
    per_view = half * half
    width = patch_ref.shape[1]
    short = 2 * channels
    wide = 2 * cells

    for source in range(sources):
        moments_ref[source * rows : (source + 1) * rows, :] = parts_ref[source, 1 : rows + 1, :]
    for source in range(sources):
        if source > 0:
            moments_ref[source * rows : source * rows + 1, :] += parts_ref[
                source - 1, rows + 1 : rows + 2, :
            ]
        if source < sources - 1:
            last = (source + 1) * rows - 1
            moments_ref[last : last + 1, :] += parts_ref[source + 1, 0:1, :]

    @pl.when(chosen_ref[0, 0] == 1)
    def _():
        moments = moments_ref[...]
        into, outof = iota((lanes, cells), 0), iota((lanes, cells), 1)
        cell = outof // channels * (2 * channels) + outof % channels
        mean_part = jnp.dot(moments, one_hot(into == cell, F32), precision=HIGHEST)
        logvar = jnp.dot(moments, one_hot(into == cell + channels, F32), precision=HIGHEST)
        latent_ref[...] = mean_part + jnp.exp(0.5 * logvar) * vae_ref[...]
        in_patch = patch_mask(per_view, half, wide, short)

        for a in range(views):
            keep_part = table_ref[0, steps_ref[a]]
            blend_part = table_ref[1, steps_ref[a]]
            moved = jnp.dot(latent_ref[...], column_ref[a], precision=HIGHEST)
            moved = jnp.dot(row_ref[a], moved, precision=HIGHEST)
            moved = jnp.concatenate([moved[:half], moved[half:]], axis=1)
            noised = keep_part * moved + blend_part * noise_ref[a * half : (a + 1) * half, :]
            patches = jnp.where(in_patch, over_patches(noised), 0.0).astype(BF16)
            tokens = jnp.dot(patches, patch_ref[...], preferred_element_type=F32)
            tokens = tokens + place_ref[...]
            shift_row = modulation_ref[a : a + 1, 0:width]
            scale_row = modulation_ref[a : a + 1, width : 2 * width]
            center = tokens - row_mean(tokens)
            variance = row_mean(center * center)
            normed = center * lax.rsqrt(variance + norm_epsilon)
            here = slice(a * per_view, (a + 1) * per_view)
            token_ref[here, :] = tokens
            mod_ref[here, :] = (normed * (1.0 + scale_row) + shift_row).astype(BF16)


def grad_kernel(blocks, views, chosen_ref, parity_ref, noise_ref, token_ref, mod_ref, modulation_ref, final_ref, *rest):
    own_fc1, own_fc2 = rest[0], rest[1]
    mine = rest[2 : 2 + blocks - 1]
    theirs = rest[1 + blocks : 2 * blocks]
    outs = rest[2 * blocks :]
    loss_ref = outs[0]
    keep_refs = outs[1 : 1 + blocks]
    send_refs = outs[1 + blocks : 1 + 2 * blocks]
    weight_ref, hidden_ref, slope_ref, pre_ref, branch_ref, grad_ref = outs[1 + 2 * blocks :]

    tokens_count, width = token_ref.shape
    wide = noise_ref.shape[1]
    half = noise_ref.shape[0] // views
    per_view = half * half
    short = wide // 2 // half
    piece = own_fc1.shape[1]
    total = piece * blocks
    entries = tokens_count * 2 * short
    parity = parity_ref[0]

    @pl.when(chosen_ref[0, 0] != 1)
    def _():
        loss_ref[...] = jnp.zeros_like(loss_ref)
        for k in range(blocks):
            keep_refs[k][...] = jnp.zeros_like(keep_refs[k])
            send_refs[k][...] = jnp.zeros_like(send_refs[k])

    @pl.when(chosen_ref[0, 0] == 1)
    def _():
        weight_ref[0, 0] = own_fc1[...]
        weight_ref[1, 0] = own_fc2[...]
        for k in range(1, blocks):
            weight_ref[parity, k] = mine[k - 1][...]
            weight_ref[1 - parity, k] = theirs[k - 1][...]
        in_patch = patch_mask(per_view, half, wide, short)

        def columns(k):
            return slice(k * piece, (k + 1) * piece)

        def view(a, loss_sum):
            here = pl.ds(a * per_view, per_view)
            gate = modulation_ref[pl.ds(a, 1), 2 * width : 3 * width]
            modulated = mod_ref[here, :]
            branch = jnp.zeros((per_view, width), F32)
            for k in range(blocks):
                x = jnp.dot(modulated, weight_ref[0, k], preferred_element_type=F32)
                square = x * x
                tanh = jnp.tanh(x * (square * (GELU_C * GELU_A) + GELU_C))
                cdf = 0.5 * tanh + 0.5
                hidden = x * cdf
                slope_ref[:, columns(k)] = cdf + (hidden * (1.0 - cdf)) * (
                    square * (6.0 * GELU_C * GELU_A) + 2.0 * GELU_C
                )
                hidden = hidden.astype(BF16)
                hidden_ref[here, columns(k)] = hidden
                branch = branch + lax.dot_general(
                    hidden, weight_ref[1, k], (((1,), (1,)), ((), ())), preferred_element_type=F32
                )
            mixed = token_ref[here, :] + gate * branch
            center = mixed - row_mean(mixed)
            variance = row_mean(center * center)
            inverse = lax.rsqrt(variance + norm_epsilon)
            normed = center * inverse
            predicted = lax.dot_general(
                normed.astype(BF16), final_ref[...], (((1,), (1,)), ((), ())),
                preferred_element_type=F32,
            )
            noise = noise_ref[pl.ds(a * half, half), :]
            residue = jnp.where(in_patch, predicted - over_patches(noise), 0.0)
            loss_sum = loss_sum + jnp.sum(residue * residue, axis=0, keepdims=True)
            grad_pred = (residue * (2.0 / entries)).astype(BF16)
            grad_normed = jnp.dot(grad_pred, final_ref[...], preferred_element_type=F32)
            grad_mixed = inverse * (
                grad_normed - row_mean(grad_normed) - normed * row_mean(grad_normed * normed)
            )
            grad_branch = (gate * grad_mixed).astype(BF16)
            branch_ref[here, :] = grad_branch
            for k in range(blocks):
                grad_hidden = jnp.dot(
                    grad_branch, weight_ref[1, k], preferred_element_type=F32
                )
                pre_ref[here, columns(k)] = (slope_ref[:, columns(k)] * grad_hidden).astype(BF16)
            return loss_sum

        loss_sum = lax.fori_loop(0, views, view, jnp.zeros((1, wide), F32), unroll=2)
        loss_ref[...] = jnp.broadcast_to(
            jnp.sum(loss_sum, keepdims=True) * (1.0 / entries), loss_ref.shape
        )

        modulated_t = mod_ref[...].T
        branch_t = branch_ref[...].T
        squares = jnp.zeros((1, piece), F32)
        for k in range(blocks):
            grad = jnp.dot(modulated_t, pre_ref[:, columns(k)], preferred_element_type=F32)
            grad_ref[0, k] = grad
            squares = squares + jnp.sum(grad * grad, axis=0, keepdims=True)
            grad = jnp.dot(branch_t, hidden_ref[:, columns(k)], preferred_element_type=F32)
            grad_ref[1, k] = grad
            squares = squares + jnp.sum(grad * grad, axis=0, keepdims=True)
        root_mean = jnp.sqrt(jnp.sum(squares, keepdims=True) / (2 * width * total))
        factor = 1.0 / (root_mean + clip_offset)
        for k in range(blocks):
            keep_refs[k][...] = grad_ref[parity, k] * factor
            send_refs[k][...] = grad_ref[1 - parity, k] * factor


VMEM = pl.BlockSpec(memory_space=pltpu.VMEM)
SMEM = pl.BlockSpec(memory_space=pltpu.SMEM)
HBM = pl.BlockSpec(memory_space=pltpu.HBM)


def prepare_call(scalars, constant, noise, weights, side):
    views, flat = noise.shape
    half = side // 2
    wide = flat // half
    cells = wide // 2
    width = weights[0].shape[1]
    inputs = [constant, noise, *weights]
    out_shape = [
        jax.ShapeDtypeStruct((16, 3 * width), F32),
        jax.ShapeDtypeStruct((wide, width), BF16),
        jax.ShapeDtypeStruct((wide, width), BF16),
        jax.ShapeDtypeStruct((half * half, width), F32),
        jax.ShapeDtypeStruct((views * half, wide), F32),
        jax.ShapeDtypeStruct((views, cells, cells), F32),
        jax.ShapeDtypeStruct((views, side, side), F32),
    ]
    return pl.pallas_call(
        partial(prepare_kernel, side),
        out_shape=out_shape,
        in_specs=[SMEM] * len(scalars) + [HBM] * len(inputs),
        out_specs=[VMEM] * len(out_shape),
        scratch_shapes=[pltpu.VMEM(v.shape, v.dtype) for v in inputs]
        + [pltpu.SemaphoreType.DMA((len(inputs),))],
        compiler_params=pltpu.CompilerParams(vmem_limit_bytes=52 << 20),
        cost_estimate=pl.CostEstimate(
            flops=1 << 27, bytes_accessed=1 << 21, transcendentals=0
        ),
        name="prepare",
    )(*scalars, *inputs)


def token_call(scalars, arrays, rows):
    parts, vae, _, patch, place = arrays[:5]
    lanes = parts.shape[2]
    side = parts.shape[0] * rows
    width = patch.shape[1]
    views = scalars[1].shape[0]
    tokens = views * place.shape[0]
    cells = vae.shape[1]
    out_shape = [
        jax.ShapeDtypeStruct((side, lanes), F32),
        jax.ShapeDtypeStruct((tokens, width), F32),
        jax.ShapeDtypeStruct((tokens, width), BF16),
    ]
    return pl.pallas_call(
        partial(token_kernel, rows),
        out_shape=out_shape,
        in_specs=[SMEM] * len(scalars) + [VMEM] * len(arrays),
        out_specs=[VMEM] * len(out_shape),
        scratch_shapes=[pltpu.VMEM((side, cells), F32)],
        compiler_params=pltpu.CompilerParams(vmem_limit_bytes=20 << 20),
        cost_estimate=pl.CostEstimate(
            flops=4 * tokens * width * cells, bytes_accessed=16 * tokens * width, transcendentals=0
        ),
        name="tokens",
    )(*scalars, *arrays)


def grad_call(chosen, parity, views, arrays, own, mine, theirs):
    blocks = len(mine) + 1
    _, token = arrays[:2]
    tokens, width = token.shape
    per_view = tokens // views
    piece = own[0].shape[1]
    total = piece * blocks
    inputs = list(arrays) + list(own) + list(mine) + list(theirs)
    out_shape = [jax.ShapeDtypeStruct((16, 128), F32)] + [
        jax.ShapeDtypeStruct((width, piece), F32)
    ] * (2 * blocks)
    return pl.pallas_call(
        partial(grad_kernel, blocks, views),
        out_shape=out_shape,
        in_specs=[SMEM] * 2 + [VMEM] * len(inputs),
        out_specs=[VMEM] * len(out_shape),
        scratch_shapes=[
            pltpu.VMEM((2, blocks, width, piece), BF16),
            pltpu.VMEM((tokens, total), BF16),
            pltpu.VMEM((per_view, total), F32),
            pltpu.VMEM((tokens, total), BF16),
            pltpu.VMEM((tokens, width), BF16),
            pltpu.VMEM((2, blocks, width, piece), F32),
        ],
        compiler_params=pltpu.CompilerParams(vmem_limit_bytes=36 << 20),
        cost_estimate=pl.CostEstimate(
            flops=10 * tokens * width * total,
            bytes_accessed=20 * width * total,
            transcendentals=tokens * total,
        ),
        name="grads",
    )(chosen, parity, *inputs)


def shift(values, axis, flip):
    count = lax.axis_size(axis)
    return lax.ppermute(values, axis, [(i, i ^ flip) for i in range(count)])


LOSS_SCALE = 64.0
NEXT = 2.0 ** (LINK_MANTISSA + 1)


def to_link(values):
    return lax.reduce_precision(values, LINK_EXPONENT, LINK_MANTISSA)


def pack_loss(loss):
    high = to_link(loss * (1.0 / LOSS_SCALE))
    rest = (loss * (1.0 / LOSS_SCALE) - high) * NEXT
    middle = to_link(rest)
    low = to_link((rest - middle) * NEXT)
    return jnp.concatenate([high, middle, low], axis=1)


def unpack_loss(packed):
    high, middle, low = jnp.split(packed.astype(F32), 3, axis=1)
    return (high + (middle + low * (1.0 / NEXT)) * (1.0 / NEXT)) * LOSS_SCALE


def per_device(
    features,
    conv_weight,
    vae_noise,
    flips,
    crops,
    tsteps,
    diffusion_noise,
    selected,
    w_patch,
    w_time,
    w_ada,
    w_fc1,
    w_fc2,
    w_final,
    noise_fc1,
    noise_fc2,
):
    groups = lax.axis_size("fsdp")
    sources = lax.axis_size("dp")
    parity = lax.axis_index("dp") % CORES
    even = parity == 0
    local_rows = features[0]
    rows, side = local_rows.shape[1], local_rows.shape[2]
    outs = conv_weight.shape[3]
    channels = outs // 2
    width, piece = w_fc1.shape
    views = flips.shape[2]

    own_kind = jnp.where(even, w_fc1, w_fc2)
    mine = [shift(own_kind, "fsdp", k) for k in range(1, groups)]

    local = local_conv(local_rows, conv_weight)
    parts = lax.all_to_all(local, "dp", split_axis=0, concat_axis=0, tiled=True)
    steps = tsteps[0, 0]
    table = jnp.asarray(noise_tables(TSTEPS))
    constant = jnp.asarray(constants(side // 2, width, w_time.shape[0]))
    modulation, patch, final, place, noise, column, row = prepare_call(
        [flips[0, 0], crops[0, 0].T, steps, table],
        constant,
        diffusion_noise[0, 0],
        lax.optimization_barrier((w_patch, w_time, w_ada, w_final.T, local))[:4],
        side,
    )
    *mine, modulation = lax.optimization_barrier((*mine, modulation))
    theirs = [shift(block, "dp", 1) for block in mine]
    own = (w_fc1, w_fc2)
    blocked = piece % 128 == 0
    if not blocked:
        joined = jnp.concatenate([own_kind] + mine, axis=1)
        other = jnp.concatenate([jnp.where(even, w_fc2, w_fc1)] + theirs, axis=1)
        own = (jnp.where(even, joined, other), jnp.where(even, other, joined))
        mine, theirs = [], []
    moments, tokens, modulated = token_call(
        [selected, steps, table],
        [parts, vae_noise.reshape(side, side * channels)]
        + [modulation, patch, place, noise, column, row],
        rows,
    )
    loss, *grads = grad_call(
        selected,
        parity.astype(jnp.int32).reshape(1),
        views,
        [noise, tokens, modulated, modulation, final],
        own,
        mine,
        theirs,
    )
    keep, send = grads[: len(grads) // 2], grads[len(grads) // 2 :]
    if not blocked:
        keep = jnp.split(keep[0], groups, axis=1)
        send = jnp.split(send[0], groups, axis=1)

    loss = loss[:, : piece // 3]
    received = [shift(block.astype(LINK), "dp", 1) for block in send]
    *received, other = lax.optimization_barrier((*received, shift(loss, "dp", 1)))
    pair = [kept + block.astype(F32) for kept, block in zip(keep, received)]
    loss = loss + other
    middle = width // 2
    halves = [[block[:middle] for block in pair], [block[middle:] for block in pair]]

    def exchange(moving, axis, flips_of):
        packed = pack_loss(loss)
        moved = [
            jnp.concatenate([moving[0], packed], axis=0).astype(LINK),
            moving[1].astype(LINK),
        ]
        moved = [shift(block, axis, flip) for block, flip in zip(moved, flips_of)]
        first, second = [block.astype(F32) for block in lax.optimization_barrier(moved)]
        size = moving[0].shape[0]
        return (first[:size], second), unpack_loss(packed) + unpack_loss(first[size:])

    bits = [1 << b for b in range(groups.bit_length() - 1)]
    for step in range(len(bits)):
        flips_of = (bits[step], bits[-1 - step])
        gone = [
            [k for k in range(groups) if k & bit and half[k] is not None]
            for half, bit in zip(halves, flips_of)
        ]
        moving = [
            jnp.concatenate([half[k] for k in ks], axis=0) for half, ks in zip(halves, gone)
        ]
        received, loss = exchange(moving, "fsdp", flips_of)
        for half, bit, ks, moved in zip(halves, flips_of, gone, received):
            for n, k in enumerate(ks):
                half[k ^ bit] = half[k ^ bit] + moved[n * middle : (n + 1) * middle]
                half[k] = None
    halves = [half[0] for half in halves]
    chips = sources // CORES
    hops = [(2 << b) - 1 for b in range(chips.bit_length() - 1)]
    for step in range(len(hops)):
        halves = [to_link(half) for half in halves]
        flips_of = (CORES * hops[step], CORES * hops[-1 - step])
        received, loss = exchange(halves, "dp", flips_of)
        halves = [half + moved for half, moved in zip(halves, received)]
    partner = [shift(half, "dp", 1) for half in halves]
    summed = jnp.concatenate(halves, axis=0)
    partner = jnp.concatenate(partner, axis=0)
    loss_all = lax.optimization_barrier(loss)[0, 0]

    selected_count = selected.shape[0] * sources * groups // 2
    sum_fc1 = jnp.where(even, summed, partner)
    sum_fc2 = jnp.where(even, partner, summed)
    update_fc1 = (sum_fc1 + noise_weight * noise_fc1) / selected_count
    update_fc2 = (sum_fc2 + noise_weight * noise_fc2) / selected_count
    latent_moments = moments.reshape(1, 1, side * side * outs)
    return (update_fc1, update_fc2, loss_all / selected_count, latent_moments)


def solution(mesh):
    in_specs = (
        P("fsdp", None, "dp", None, None),
        P(),
        P("dp", "fsdp", None),
        P("dp", "fsdp", None),
        P("dp", "fsdp", None, None),
        P("dp", "fsdp", None),
        P("dp", "fsdp", None, None),
        P("dp", "fsdp"),
        P(),
        P(),
        P(),
        P(None, "fsdp"),
        P(None, "fsdp"),
        P(),
        P(None, "fsdp"),
        P(None, "fsdp"),
    )
    out_specs = (P(None, "fsdp"), P(None, "fsdp"), P(), P("dp", "fsdp", None))
    return jax.shard_map(
        per_device, mesh=mesh, in_specs=in_specs, out_specs=out_specs, check_vma=False
    )
```

```python
from functools import partial
import math

import numpy as np

import jax
import jax.numpy as jnp
from jax import lax
from jax.experimental import pallas as pl
from jax.experimental.pallas import tpu as pltpu
from jax.sharding import PartitionSpec as P


TSTEPS = 1000
CORES = 2

clip_offset = 1e-05
noise_weight = 16.0
norm_epsilon = 1e-06

LINK = jnp.float16
LINK_EXPONENT, LINK_MANTISSA = jnp.finfo(LINK).nexp, jnp.finfo(LINK).nmant
HIGHEST = lax.Precision.HIGHEST
F32 = jnp.float32
BF16 = jnp.bfloat16
GELU_C = math.sqrt(2.0 / math.pi)
GELU_A = 0.044715


def noise_tables(horizon):
    beta = np.linspace(0.0001, 0.02, horizon, dtype=np.float32)
    alpha_bar = np.cumprod(np.float32(1.0) - beta, dtype=np.float32)
    return np.stack([np.sqrt(alpha_bar), np.sqrt(np.float32(1.0) - alpha_bar)])


def position_table(side_cells, width):
    quarter = width // 4
    frequency = np.float32(1.0) / np.power(
        np.float32(10000.0), np.arange(quarter, dtype=np.float32) / np.float32(quarter)
    )
    angles = np.arange(side_cells, dtype=np.float32)[:, None] * frequency[None, :]
    line = np.concatenate([np.sin(angles), np.cos(angles)], axis=1).astype(np.float32)
    blank = np.zeros_like(line)
    return np.stack(
        [np.concatenate([line, blank], axis=1), np.concatenate([blank, line], axis=1)]
    )


def constants(side_cells, width, features):
    half = features // 2
    rates = np.exp(-math.log(10000.0) * np.arange(half, dtype=np.float32) / np.float32(half))
    lines = position_table(side_cells, width)
    rates = np.pad(rates.astype(np.float32), (0, width - half))
    return np.concatenate([lines, np.broadcast_to(rates, lines[:1].shape)]).astype(np.float32)


def iota(shape, axis):
    return lax.broadcasted_iota(jnp.int32, shape, axis)


def one_hot(condition, dtype):
    return jnp.where(condition, 1.0, 0.0).astype(dtype)


def split_float(values):
    high = values.astype(BF16)
    rest = values - high.astype(F32)
    middle = rest.astype(BF16)
    return high, middle, (rest - middle.astype(F32)).astype(BF16)


def conv_kernel(rows, side, outs, feat_ref, weight_ref, out_ref):
    images = out_ref.shape[0]
    cells, channels = feat_ref.shape
    lanes = side * outs
    taps = 128
    weights = jnp.concatenate(
        [weight_ref[...], jnp.zeros((taps - 9 * outs, channels), BF16)], axis=0
    )
    products = lax.dot_general(
        feat_ref[...], weights, (((1,), (1,)), ((), ())), preferred_element_type=F32
    )
    zero_row = jnp.zeros((1, taps), F32)
    before = jnp.concatenate([zero_row, products[: cells - 1]], axis=0)
    after = jnp.concatenate([products[1:], zero_row], axis=0)
    column = iota((cells, taps), 0) % side
    tap = iota((cells, taps), 1) // outs % 3
    chosen = jnp.where(
        tap == 1,
        products,
        jnp.where(
            tap == 0,
            jnp.where(column == 0, 0.0, before),
            jnp.where(column == side - 1, 0.0, after),
        ),
    )
    source, target = iota((taps, 3 * lanes), 0), iota((taps, 3 * lanes), 1)
    wanted = (source // (3 * outs) == target // lanes) & (source % outs == target % outs)
    spread = one_hot(wanted & (source < 9 * outs), BF16)
    wide = jnp.zeros((cells, 3 * lanes), F32)
    for part in split_float(chosen):
        wide = wide + jnp.dot(part, spread, preferred_element_type=F32)
    own = iota((cells, lanes), 1) // outs == iota((cells, lanes), 0) % side
    out_ref[...] = jnp.zeros(out_ref.shape, F32)
    for row_tap in range(3):
        placed = jnp.where(own, wide[:, row_tap * lanes : (row_tap + 1) * lanes], 0.0)
        line = jnp.sum(placed.reshape(images * rows, side, lanes), axis=1)
        line = line.reshape(images, rows, lanes)
        start = 2 - row_tap
        for s in range(images):
            out_ref[s, start : start + rows, :] += line[s]


def local_conv(features, conv_weight):
    images, rows, side, channels = features.shape
    outs = conv_weight.shape[3]
    lanes = side * outs
    padded = -(-(rows + 2) // 8) * 8
    weight = conv_weight.transpose(0, 1, 3, 2).reshape(9 * outs, channels)
    steps = 2 if images % 2 == 0 else 1
    cells = images * rows * side
    return pl.pallas_call(
        partial(conv_kernel, rows, side, outs),
        out_shape=jax.ShapeDtypeStruct((images, padded, lanes), F32),
        grid=(steps,),
        in_specs=[
            pl.BlockSpec((cells // steps, channels), lambda i: (i, 0)),
            pl.BlockSpec((9 * outs, channels), lambda i: (0, 0)),
        ],
        out_specs=pl.BlockSpec((images // steps, padded, lanes), lambda i: (i, 0, 0)),
        compiler_params=pltpu.CompilerParams(vmem_limit_bytes=56 << 20),
        cost_estimate=pl.CostEstimate(
            flops=2 * images * rows * lanes * channels * 9,
            bytes_accessed=features.size * 2,
            transcendentals=0,
        ),
        name="local_conv",
    )(features.reshape(cells, channels), weight)


def row_mean(values):
    return jnp.sum(values, axis=-1, keepdims=True) * (1.0 / values.shape[-1])


def patch_mask(per_view, half, wide, short):
    cells = wide // 2
    return iota((per_view, wide), 1) % cells // short == iota((per_view, wide), 0) % half


def over_patches(values):
    half, wide = values.shape
    return jnp.broadcast_to(values[:, None, :], (half, half, wide)).reshape(half * half, wide)


def prepare_kernel(
    side,
    flips_ref,
    crops_ref,
    steps_ref,
    table_ref,
    constant_hbm,
    noise_hbm,
    w_patch_hbm,
    w_time_hbm,
    w_ada_hbm,
    w_final_hbm,
    modulation_ref,
    patch_ref,
    final_ref,
    place_ref,
    noise_ref,
    column_ref,
    row_ref,
    constant_ref,
    raw_noise_ref,
    w_patch_ref,
    w_time_ref,
    w_ada_ref,
    w_final_ref,
    sems,
):
    views = steps_ref.shape[0]
    half = side // 2
    wide = noise_ref.shape[1]
    cells = wide // 2
    short = cells // half
    channels = short // 2
    width = w_patch_ref.shape[1]
    half_freq = w_time_ref.shape[0] // 2
    sources = (constant_hbm, noise_hbm, w_patch_hbm, w_time_hbm, w_ada_hbm, w_final_hbm)
    targets = (constant_ref, raw_noise_ref, w_patch_ref, w_time_ref, w_ada_ref, w_final_ref)
    copies = [
        pltpu.make_async_copy(source, target, sems.at[n])
        for n, (source, target) in enumerate(zip(sources, targets))
    ]
    for copy in copies:
        copy.start()

    source, target = iota((cells, cells), 0), iota((cells, cells), 1)
    target_row, source_row = iota((side, side), 0), iota((side, side), 1)
    for a in range(views):
        column = target // channels + (crops_ref[1, a] - 2)
        valid = (column >= 0) & (column < side)
        column = jnp.where(flips_ref[a] == 1, side - 1 - column, column)
        column_ref[a] = one_hot(
            valid & (source == column * channels + target % channels), F32
        )
        wanted = target_row % half * 2 + target_row // half + (crops_ref[0, a] - 2)
        row_ref[a] = one_hot(source_row == wanted, F32)

    for copy in copies:
        copy.wait()
    steps = jnp.zeros((modulation_ref.shape[0], half_freq), F32)
    for a in range(views):
        steps = jnp.where(iota(steps.shape, 0) == a, steps_ref[a].astype(F32), steps)
    phases = steps * constant_ref[2, 0:1, :half_freq]
    stamp = jnp.concatenate([jnp.cos(phases), jnp.sin(phases)], axis=1).astype(BF16)
    conditioning = jnp.dot(stamp, w_time_ref[...], preferred_element_type=F32)
    conditioning = conditioning * (1.0 / (1.0 + jnp.exp(-conditioning)))
    modulation_ref[...] = jnp.dot(
        conditioning.astype(BF16), w_ada_ref[...], preferred_element_type=F32
    )
    lane, entry = iota((wide, 2 * short), 0), iota((wide, 2 * short), 1)
    spread = one_hot(lane // cells * short + lane % short == entry, BF16)
    patch_ref[...] = jnp.dot(spread, w_patch_ref[...], preferred_element_type=F32).astype(BF16)
    final_ref[...] = jnp.dot(spread, w_final_ref[...], preferred_element_type=F32).astype(BF16)
    place_ref[...] = (
        jnp.broadcast_to(constant_ref[0][:, None, :], (half, half, width))
        + jnp.broadcast_to(constant_ref[1][None, :, :], (half, half, width))
    ).reshape(half * half, width)
    for a in range(views):
        for line in range(half):
            n = a * half + line
            noise_ref[n : n + 1, :] = raw_noise_ref[a : a + 1, line * wide : (line + 1) * wide]


def token_kernel(
    rows,
    chosen_ref,
    steps_ref,
    table_ref,
    parts_ref,
    vae_ref,
    modulation_ref,
    patch_ref,
    place_ref,
    noise_ref,
    column_ref,
    row_ref,
    moments_ref,
    token_ref,
    mod_ref,
    latent_ref,
):
    sources = parts_ref.shape[0]
    lanes = parts_ref.shape[2]
    side = sources * rows
    channels = vae_ref.shape[1] // side
    cells = side * channels
    views = steps_ref.shape[0]
    half = side // 2
    per_view = half * half
    width = patch_ref.shape[1]
    short = 2 * channels
    wide = 2 * cells

    for source in range(sources):
        moments_ref[source * rows : (source + 1) * rows, :] = parts_ref[source, 1 : rows + 1, :]
    for source in range(sources):
        if source > 0:
            moments_ref[source * rows : source * rows + 1, :] += parts_ref[
                source - 1, rows + 1 : rows + 2, :
            ]
        if source < sources - 1:
            last = (source + 1) * rows - 1
            moments_ref[last : last + 1, :] += parts_ref[source + 1, 0:1, :]

    @pl.when(chosen_ref[0, 0] == 1)
    def _():
        moments = moments_ref[...]
        into, outof = iota((lanes, cells), 0), iota((lanes, cells), 1)
        cell = outof // channels * (2 * channels) + outof % channels
        mean_part = jnp.dot(moments, one_hot(into == cell, F32), precision=HIGHEST)
        logvar = jnp.dot(moments, one_hot(into == cell + channels, F32), precision=HIGHEST)
        latent_ref[...] = mean_part + jnp.exp(0.5 * logvar) * vae_ref[...]
        in_patch = patch_mask(per_view, half, wide, short)

        for a in range(views):
            keep_part = table_ref[0, steps_ref[a]]
            blend_part = table_ref[1, steps_ref[a]]
            moved = jnp.dot(latent_ref[...], column_ref[a], precision=HIGHEST)
            moved = jnp.dot(row_ref[a], moved, precision=HIGHEST)
            moved = jnp.concatenate([moved[:half], moved[half:]], axis=1)
            noised = keep_part * moved + blend_part * noise_ref[a * half : (a + 1) * half, :]
            patches = jnp.where(in_patch, over_patches(noised), 0.0).astype(BF16)
            tokens = jnp.dot(patches, patch_ref[...], preferred_element_type=F32)
            tokens = tokens + place_ref[...]
            shift_row = modulation_ref[a : a + 1, 0:width]
            scale_row = modulation_ref[a : a + 1, width : 2 * width]
            center = tokens - row_mean(tokens)
            variance = row_mean(center * center)
            normed = center * lax.rsqrt(variance + norm_epsilon)
            here = slice(a * per_view, (a + 1) * per_view)
            token_ref[here, :] = tokens
            mod_ref[here, :] = (normed * (1.0 + scale_row) + shift_row).astype(BF16)


def grad_kernel(blocks, views, chosen_ref, parity_ref, noise_ref, token_ref, mod_ref, modulation_ref, final_ref, *rest):
    own_fc1, own_fc2 = rest[0], rest[1]
    mine = rest[2 : 2 + blocks - 1]
    theirs = rest[1 + blocks : 2 * blocks]
    outs = rest[2 * blocks :]
    loss_ref = outs[0]
    keep_refs = outs[1 : 1 + blocks]
    send_refs = outs[1 + blocks : 1 + 2 * blocks]
    weight_ref, hidden_ref, slope_ref, pre_ref, branch_ref, grad_ref = outs[1 + 2 * blocks :]

    tokens_count, width = token_ref.shape
    wide = noise_ref.shape[1]
    half = noise_ref.shape[0] // views
    per_view = half * half
    short = wide // 2 // half
    piece = own_fc1.shape[1]
    total = piece * blocks
    entries = tokens_count * 2 * short
    parity = parity_ref[0]

    @pl.when(chosen_ref[0, 0] != 1)
    def _():
        loss_ref[...] = jnp.zeros_like(loss_ref)
        for k in range(blocks):
            keep_refs[k][...] = jnp.zeros_like(keep_refs[k])
            send_refs[k][...] = jnp.zeros_like(send_refs[k])

    @pl.when(chosen_ref[0, 0] == 1)
    def _():
        weight_ref[0, 0] = own_fc1[...]
        weight_ref[1, 0] = own_fc2[...]
        for k in range(1, blocks):
            weight_ref[parity, k] = mine[k - 1][...]
            weight_ref[1 - parity, k] = theirs[k - 1][...]
        in_patch = patch_mask(per_view, half, wide, short)

        def columns(k):
            return slice(k * piece, (k + 1) * piece)

        def view(a, loss_sum):
            here = pl.ds(a * per_view, per_view)
            gate = modulation_ref[pl.ds(a, 1), 2 * width : 3 * width]
            modulated = mod_ref[here, :]
            branch = jnp.zeros((per_view, width), F32)
            for k in range(blocks):
                x = jnp.dot(modulated, weight_ref[0, k], preferred_element_type=F32)
                square = x * x
                tanh = jnp.tanh(x * (square * (GELU_C * GELU_A) + GELU_C))
                cdf = 0.5 * tanh + 0.5
                hidden = x * cdf
                slope_ref[:, columns(k)] = cdf + (hidden * (1.0 - cdf)) * (
                    square * (6.0 * GELU_C * GELU_A) + 2.0 * GELU_C
                )
                hidden = hidden.astype(BF16)
                hidden_ref[here, columns(k)] = hidden
                branch = branch + lax.dot_general(
                    hidden, weight_ref[1, k], (((1,), (1,)), ((), ())), preferred_element_type=F32
                )
            mixed = token_ref[here, :] + gate * branch
            center = mixed - row_mean(mixed)
            variance = row_mean(center * center)
            inverse = lax.rsqrt(variance + norm_epsilon)
            normed = center * inverse
            predicted = lax.dot_general(
                normed.astype(BF16), final_ref[...], (((1,), (1,)), ((), ())),
                preferred_element_type=F32,
            )
            noise = noise_ref[pl.ds(a * half, half), :]
            residue = jnp.where(in_patch, predicted - over_patches(noise), 0.0)
            loss_sum = loss_sum + jnp.sum(residue * residue, axis=0, keepdims=True)
            grad_pred = (residue * (2.0 / entries)).astype(BF16)
            grad_normed = jnp.dot(grad_pred, final_ref[...], preferred_element_type=F32)
            grad_mixed = inverse * (
                grad_normed - row_mean(grad_normed) - normed * row_mean(grad_normed * normed)
            )
            grad_branch = (gate * grad_mixed).astype(BF16)
            branch_ref[here, :] = grad_branch
            for k in range(blocks):
                grad_hidden = jnp.dot(
                    grad_branch, weight_ref[1, k], preferred_element_type=F32
                )
                pre_ref[here, columns(k)] = (slope_ref[:, columns(k)] * grad_hidden).astype(BF16)
            return loss_sum

        loss_sum = lax.fori_loop(0, views, view, jnp.zeros((1, wide), F32), unroll=2)
        loss_ref[...] = jnp.broadcast_to(
            jnp.sum(loss_sum, keepdims=True) * (1.0 / entries), loss_ref.shape
        )

        modulated_t = mod_ref[...].T
        branch_t = branch_ref[...].T
        squares = jnp.zeros((1, piece), F32)
        for k in range(blocks):
            grad = jnp.dot(modulated_t, pre_ref[:, columns(k)], preferred_element_type=F32)
            grad_ref[0, k] = grad
            squares = squares + jnp.sum(grad * grad, axis=0, keepdims=True)
            grad = jnp.dot(branch_t, hidden_ref[:, columns(k)], preferred_element_type=F32)
            grad_ref[1, k] = grad
            squares = squares + jnp.sum(grad * grad, axis=0, keepdims=True)
        root_mean = jnp.sqrt(jnp.sum(squares, keepdims=True) / (2 * width * total))
        factor = 1.0 / (root_mean + clip_offset)
        for k in range(blocks):
            keep_refs[k][...] = grad_ref[parity, k] * factor
            send_refs[k][...] = grad_ref[1 - parity, k] * factor


VMEM = pl.BlockSpec(memory_space=pltpu.VMEM)
SMEM = pl.BlockSpec(memory_space=pltpu.SMEM)
HBM = pl.BlockSpec(memory_space=pltpu.HBM)


def prepare_call(scalars, constant, noise, weights, side):
    views, flat = noise.shape
    half = side // 2
    wide = flat // half
    cells = wide // 2
    width = weights[0].shape[1]
    inputs = [constant, noise, *weights]
    out_shape = [
        jax.ShapeDtypeStruct((16, 3 * width), F32),
        jax.ShapeDtypeStruct((wide, width), BF16),
        jax.ShapeDtypeStruct((wide, width), BF16),
        jax.ShapeDtypeStruct((half * half, width), F32),
        jax.ShapeDtypeStruct((views * half, wide), F32),
        jax.ShapeDtypeStruct((views, cells, cells), F32),
        jax.ShapeDtypeStruct((views, side, side), F32),
    ]
    return pl.pallas_call(
        partial(prepare_kernel, side),
        out_shape=out_shape,
        in_specs=[SMEM] * len(scalars) + [HBM] * len(inputs),
        out_specs=[VMEM] * len(out_shape),
        scratch_shapes=[pltpu.VMEM(v.shape, v.dtype) for v in inputs]
        + [pltpu.SemaphoreType.DMA((len(inputs),))],
        compiler_params=pltpu.CompilerParams(vmem_limit_bytes=52 << 20),
        cost_estimate=pl.CostEstimate(
            flops=1 << 27, bytes_accessed=1 << 21, transcendentals=0
        ),
        name="prepare",
    )(*scalars, *inputs)


def token_call(scalars, arrays, rows):
    parts, vae, _, patch, place = arrays[:5]
    lanes = parts.shape[2]
    side = parts.shape[0] * rows
    width = patch.shape[1]
    views = scalars[1].shape[0]
    tokens = views * place.shape[0]
    cells = vae.shape[1]
    out_shape = [
        jax.ShapeDtypeStruct((side, lanes), F32),
        jax.ShapeDtypeStruct((tokens, width), F32),
        jax.ShapeDtypeStruct((tokens, width), BF16),
    ]
    return pl.pallas_call(
        partial(token_kernel, rows),
        out_shape=out_shape,
        in_specs=[SMEM] * len(scalars) + [VMEM] * len(arrays),
        out_specs=[VMEM] * len(out_shape),
        scratch_shapes=[pltpu.VMEM((side, cells), F32)],
        compiler_params=pltpu.CompilerParams(vmem_limit_bytes=20 << 20),
        cost_estimate=pl.CostEstimate(
            flops=4 * tokens * width * cells, bytes_accessed=16 * tokens * width, transcendentals=0
        ),
        name="tokens",
    )(*scalars, *arrays)


def grad_call(chosen, parity, views, arrays, own, mine, theirs):
    blocks = len(mine) + 1
    _, token = arrays[:2]
    tokens, width = token.shape
    per_view = tokens // views
    piece = own[0].shape[1]
    total = piece * blocks
    inputs = list(arrays) + list(own) + list(mine) + list(theirs)
    out_shape = [jax.ShapeDtypeStruct((16, 128), F32)] + [
        jax.ShapeDtypeStruct((width, piece), F32)
    ] * (2 * blocks)
    return pl.pallas_call(
        partial(grad_kernel, blocks, views),
        out_shape=out_shape,
        in_specs=[SMEM] * 2 + [VMEM] * len(inputs),
        out_specs=[VMEM] * len(out_shape),
        scratch_shapes=[
            pltpu.VMEM((2, blocks, width, piece), BF16),
            pltpu.VMEM((tokens, total), BF16),
            pltpu.VMEM((per_view, total), F32),
            pltpu.VMEM((tokens, total), BF16),
            pltpu.VMEM((tokens, width), BF16),
            pltpu.VMEM((2, blocks, width, piece), F32),
        ],
        compiler_params=pltpu.CompilerParams(vmem_limit_bytes=36 << 20),
        cost_estimate=pl.CostEstimate(
            flops=10 * tokens * width * total,
            bytes_accessed=20 * width * total,
            transcendentals=tokens * total,
        ),
        name="grads",
    )(chosen, parity, *inputs)


def shift(values, axis, flip):
    count = lax.axis_size(axis)
    return lax.ppermute(values, axis, [(i, i ^ flip) for i in range(count)])


LOSS_SCALE = 64.0
NEXT = 2.0 ** (LINK_MANTISSA + 1)


def to_link(values):
    return lax.reduce_precision(values, LINK_EXPONENT, LINK_MANTISSA)


def pack_loss(loss):
    high = to_link(loss * (1.0 / LOSS_SCALE))
    rest = (loss * (1.0 / LOSS_SCALE) - high) * NEXT
    middle = to_link(rest)
    low = to_link((rest - middle) * NEXT)
    return jnp.concatenate([high, middle, low], axis=1)


def unpack_loss(packed):
    high, middle, low = jnp.split(packed.astype(F32), 3, axis=1)
    return (high + (middle + low * (1.0 / NEXT)) * (1.0 / NEXT)) * LOSS_SCALE


def per_device(
    features,
    conv_weight,
    vae_noise,
    flips,
    crops,
    tsteps,
    diffusion_noise,
    selected,
    w_patch,
    w_time,
    w_ada,
    w_fc1,
    w_fc2,
    w_final,
    noise_fc1,
    noise_fc2,
):
    groups = lax.axis_size("fsdp")
    sources = lax.axis_size("dp")
    parity = lax.axis_index("dp") % CORES
    even = parity == 0
    local_rows = features[0]
    rows, side = local_rows.shape[1], local_rows.shape[2]
    outs = conv_weight.shape[3]
    channels = outs // 2
    width, piece = w_fc1.shape
    views = flips.shape[2]

    own_kind = jnp.where(even, w_fc1, w_fc2)
    mine = [shift(own_kind, "fsdp", k) for k in range(1, groups)]

    local = local_conv(local_rows, conv_weight)
    parts = lax.all_to_all(local, "dp", split_axis=0, concat_axis=0, tiled=True)
    steps = tsteps[0, 0]
    table = jnp.asarray(noise_tables(TSTEPS))
    constant = jnp.asarray(constants(side // 2, width, w_time.shape[0]))
    modulation, patch, final, place, noise, column, row = prepare_call(
        [flips[0, 0], crops[0, 0].T, steps, table],
        constant,
        diffusion_noise[0, 0],
        lax.optimization_barrier((w_patch, w_time, w_ada, w_final.T, local))[:4],
        side,
    )
    *mine, modulation = lax.optimization_barrier((*mine, modulation))
    theirs = [shift(block, "dp", 1) for block in mine]
    own = (w_fc1, w_fc2)
    blocked = piece % 128 == 0
    if not blocked:
        joined = jnp.concatenate([own_kind] + mine, axis=1)
        other = jnp.concatenate([jnp.where(even, w_fc2, w_fc1)] + theirs, axis=1)
        own = (jnp.where(even, joined, other), jnp.where(even, other, joined))
        mine, theirs = [], []
    moments, tokens, modulated = token_call(
        [selected, steps, table],
        [parts, vae_noise.reshape(side, side * channels)]
        + [modulation, patch, place, noise, column, row],
        rows,
    )
    loss, *grads = grad_call(
        selected,
        parity.astype(jnp.int32).reshape(1),
        views,
        [noise, tokens, modulated, modulation, final],
        own,
        mine,
        theirs,
    )
    keep, send = grads[: len(grads) // 2], grads[len(grads) // 2 :]
    if not blocked:
        keep = jnp.split(keep[0], groups, axis=1)
        send = jnp.split(send[0], groups, axis=1)

    loss = loss[:, : piece // 3]
    received = [shift(block.astype(LINK), "dp", 1) for block in send]
    *received, other = lax.optimization_barrier((*received, shift(loss, "dp", 1)))
    pair = [kept + block.astype(F32) for kept, block in zip(keep, received)]
    loss = loss + other
    middle = width // 2
    halves = [[block[:middle] for block in pair], [block[middle:] for block in pair]]

    def exchange(moving, axis, flips_of):
        packed = pack_loss(loss)
        moved = [
            jnp.concatenate([moving[0], packed], axis=0).astype(LINK),
            moving[1].astype(LINK),
        ]
        moved = [shift(block, axis, flip) for block, flip in zip(moved, flips_of)]
        first, second = [block.astype(F32) for block in lax.optimization_barrier(moved)]
        size = moving[0].shape[0]
        return (first[:size], second), unpack_loss(packed) + unpack_loss(first[size:])

    bits = [1 << b for b in range(groups.bit_length() - 1)]
    for step in range(len(bits)):
        flips_of = (bits[step], bits[-1 - step])
        gone = [
            [k for k in range(groups) if k & bit and half[k] is not None]
            for half, bit in zip(halves, flips_of)
        ]
        moving = [
            jnp.concatenate([half[k] for k in ks], axis=0) for half, ks in zip(halves, gone)
        ]
        received, loss = exchange(moving, "fsdp", flips_of)
        for half, bit, ks, moved in zip(halves, flips_of, gone, received):
            for n, k in enumerate(ks):
                half[k ^ bit] = half[k ^ bit] + moved[n * middle : (n + 1) * middle]
                half[k] = None
    halves = [half[0] for half in halves]
    chips = sources // CORES
    hops = [(2 << b) - 1 for b in range(chips.bit_length() - 1)]
    for step in range(len(hops)):
        halves = [to_link(half) for half in halves]
        flips_of = (CORES * hops[step], CORES * hops[-1 - step])
        received, loss = exchange(halves, "dp", flips_of)
        halves = [half + moved for half, moved in zip(halves, received)]
    partner = [shift(half, "dp", 1) for half in halves]
    summed = jnp.concatenate(halves, axis=0)
    partner = jnp.concatenate(partner, axis=0)
    loss_all = lax.optimization_barrier(loss)[0, 0]

    selected_count = selected.shape[0] * sources * groups // 2
    sum_fc1 = jnp.where(even, summed, partner)
    sum_fc2 = jnp.where(even, partner, summed)
    update_fc1 = (sum_fc1 + noise_weight * noise_fc1) / selected_count
    update_fc2 = (sum_fc2 + noise_weight * noise_fc2) / selected_count
    latent_moments = moments.reshape(1, 1, side * side * outs)
    return (update_fc1, update_fc2, loss_all / selected_count, latent_moments)


def solution(mesh):
    in_specs = (
        P("fsdp", None, "dp", None, None),
        P(),
        P("dp", "fsdp", None),
        P("dp", "fsdp", None),
        P("dp", "fsdp", None, None),
        P("dp", "fsdp", None),
        P("dp", "fsdp", None, None),
        P("dp", "fsdp"),
        P(),
        P(),
        P(),
        P(None, "fsdp"),
        P(None, "fsdp"),
        P(),
        P(None, "fsdp"),
        P(None, "fsdp"),
    )
    out_specs = (P(None, "fsdp"), P(None, "fsdp"), P(), P("dp", "fsdp", None))
    return jax.shard_map(
        per_device, mesh=mesh, in_specs=in_specs, out_specs=out_specs, check_vma=False
    )
```
